768 devices in a mesh: dp: 96 (over z, x, core), mp: 8 (over y).
Axes of the slice: x: 4, y: 8, z: 12, core: 2. Of those that a mesh axis runs over, the one named last changes fastest.
Arguments:
- vision_rows: bfloat16 [24576, 1024], P('dp'), may hold values from -6 to 6
- image_count: int32 [768], P('dp'), may hold values from 0 to 4
- proj_flat: bfloat16 [36864, 128], P(('dp', 'mp')), may hold values from -0.1875 to 0.1875
- text_embeds: bfloat16 [73728, 4096], P(('dp', 'mp')), may hold values from -6 to 6
- norm_gain: float32 [4096], replicated, may hold values from 0.1 to 1.9
- q_weight: bfloat16 [4096, 4096], P(None, 'mp'), may hold values from -0.09375 to 0.09375
- q_grad: bfloat16 [98304, 4096], P('dp', 'mp'), may hold values from -6 to 6
Outputs:
- text_grad: bfloat16 [73728, 4096], P(('dp', 'mp'))
- proj_grad: float32 [36864, 128], P(('dp', 'mp'))
The draws below stay inside these ranges and needn't reach their ends.
Inputs may be any that keep to these rules, and one draw needn't show every extreme that they name: Slot s of device k holds an image when s < image_count[k]; other slots are padding.
All inputs are finite; a program needn't handle non-finite values.
Results may differ from the reference program's by a relative error of at most 0.014.
Values may be sent and summed in bfloat16 or wider, within the bound.
A program may use at most 64 MiB of HBM per device.

```python
import jax
import jax.numpy as jnp
from jax import lax

D = 4096
ENC = 1024
IMG_MAX = 4
PATCH = 8
TEXT_DEV = 96
IMG_ROWS = 32
ROWS_DEV = 128
PROJ_ROWS = 48
N_DP = 96
N_MP = 8


def plant(drawn, own_key, least, largest):
    longest = drawn.shape.index(max(drawn.shape))
    spots = []
    for shift in (0, 1):
        where = [jax.random.randint(jax.random.fold_in(own_key, axis), (), 0, length) for axis, length in enumerate(drawn.shape)]
        where[longest] = (where[longest] + shift) % drawn.shape[longest]
        spots.append(tuple(where))
    return drawn.at[spots[0]].set(least).at[spots[1]].set(largest)


def block_scale(key, extent, cuts, smallest, high):
    level = 1.0
    for position, blocks in cuts:
        heights = jax.random.uniform(jax.random.fold_in(jax.random.fold_in(key, 6), position), (blocks,), jnp.float32, smallest / len(cuts), high / len(cuts))
        level = level * jnp.repeat(jnp.exp(heights), extent[position] // blocks).reshape((-1,) + (1,) * (len(extent) - 1 - position))
    return level


def bell_draw(own_key, dims, deviation, most, split=(), kind=jnp.bfloat16):
    gain = block_scale(own_key, dims, split, -0.22, 0.18) if split else 1.0
    array = jax.random.normal(own_key, dims, jnp.float32) * deviation * gain
    return jnp.minimum(jnp.maximum(array, -most), most).astype(kind)


def setup_inputs(seed: int = 0) -> dict:
    streams_of = jax.random.split(jax.random.key(seed), 8)
    vision_rows = bell_draw(streams_of[0], (N_DP * N_MP * IMG_ROWS, ENC), 1.0, 6.0, ((0, 96),))
    image_count = plant(jax.random.randint(streams_of[1], (N_DP * N_MP,), 0, IMG_MAX + 1), jax.random.fold_in(streams_of[1], 1), 0, IMG_MAX).astype(jnp.int32)
    proj_flat = bell_draw(streams_of[2], (N_DP * N_MP * PROJ_ROWS, 128), ENC ** -0.5, 0.1875, ((0, 768),))
    text_embeds = bell_draw(streams_of[3], (N_DP * N_MP * TEXT_DEV, D), 1.0, 6.0, ((0, 768),))
    norm_gain = jnp.clip(1.0 + 0.18 * jax.random.normal(streams_of[4], (D,), jnp.float32), 0.1, 1.9)
    q_weight = bell_draw(streams_of[5], (D, D), D ** -0.5, 0.09375, ((1, 8),))
    q_grad = bell_draw(streams_of[6], (N_DP * N_MP * ROWS_DEV, D), 1.0, 6.0, ((0, 96), (1, 8)))
    return {"vision_rows": vision_rows, "image_count": image_count, "proj_flat": proj_flat, "text_embeds": text_embeds, "norm_gain": norm_gain, "q_weight": q_weight, "q_grad": q_grad}


norm_eps = 1e-05

def reference(vision_rows, image_count, proj_flat, text_embeds, norm_gain, q_weight, q_grad):
    block_cols = D // N_MP
    used_count = ENC * block_cols
    stored = proj_flat.reshape(N_DP, N_MP, PROJ_ROWS * 128).transpose(1, 0, 2)
    stored = stored.reshape(N_MP, N_DP * PROJ_ROWS * 128)[:, :used_count]
    proj_weight = stored.reshape(N_MP, ENC, block_cols).transpose(1, 0, 2).reshape(ENC, D)
    image_embed = jnp.dot(vision_rows, proj_weight, preferred_element_type=jnp.float32).astype(jnp.bfloat16)
    image_blocks = image_embed.reshape(N_DP * N_MP, IMG_ROWS, D)
    text_blocks = text_embeds.reshape(N_DP * N_MP, TEXT_DEV, D)
    decoder_in = jnp.concatenate([image_blocks, text_blocks], axis=1).reshape(-1, D)
    inputs = decoder_in.astype(jnp.float32)
    inv_rms = lax.rsqrt(lax.optimization_barrier(jnp.mean(inputs * inputs, axis=-1, keepdims=True)) + norm_eps)
    norm_grad = jnp.zeros(inputs.shape, jnp.float32)
    for member in range(N_MP):
        left = q_grad[:, member * block_cols:(member + 1) * block_cols]
        right = q_weight[:, member * block_cols:(member + 1) * block_cols]
        term = jnp.dot(left, right.T, preferred_element_type=jnp.float32).astype(jnp.bfloat16)
        term = lax.optimization_barrier(term)
        norm_grad = norm_grad + term.astype(jnp.float32)
    scaled = norm_gain[None, :] * norm_grad
    inner_mean = lax.optimization_barrier(jnp.mean(scaled * inputs, axis=-1, keepdims=True))
    input_grad = inv_rms * scaled - inputs * inv_rms ** 3 * inner_mean
    grad_blocks = input_grad.reshape(N_DP * N_MP, ROWS_DEV, D)
    text_grad = grad_blocks[:, IMG_ROWS:, :].reshape(-1, D).astype(jnp.bfloat16)
    live_slots = jnp.arange(IMG_MAX, dtype=jnp.int32)[None, :] < image_count[:, None]
    live_rows = jnp.repeat(live_slots, PATCH, axis=1)
    image_grad = jnp.where(live_rows[:, :, None], grad_blocks[:, :IMG_ROWS, :], 0.0)
    image_grad = image_grad.reshape(-1, D).astype(jnp.bfloat16)
    grad_scale = 1.0 / jnp.sqrt(jnp.float32(N_DP * N_MP * IMG_ROWS))
    proj_full = jnp.dot(vision_rows.T, image_grad, preferred_element_type=jnp.float32) * grad_scale
    flat_blocks = proj_full.reshape(ENC, N_MP, block_cols).transpose(1, 0, 2).reshape(N_MP, used_count)
    flat_blocks = jnp.pad(flat_blocks, ((0, 0), (0, N_DP * PROJ_ROWS * 128 - used_count)))
    proj_grad = flat_blocks.reshape(N_MP, N_DP, PROJ_ROWS * 128).transpose(1, 0, 2)
    proj_grad = proj_grad.reshape(N_DP * N_MP * PROJ_ROWS, 128)
    return (text_grad, proj_grad)
```

```python
import functools

import jax
import jax.numpy as jnp
from jax import lax
from jax.experimental import pallas as pl
from jax.experimental.pallas import tpu as pltpu
from jax.sharding import Mesh
from jax.sharding import PartitionSpec as P

IMG_MAX = 4
PATCH = 8
IMG = IMG_MAX * PATCH
LANES = 128
DP = ("dp_0", "dp_1", "dp_2")
DP_MP = ("dp_0", "dp_1", "dp_2", "mp")
EPS = 1e-05
MESH = pl.DeviceIdType.MESH
F32 = jnp.float32
BF16 = jnp.bfloat16


def dot_nt(a, b):
    return lax.dot_general(a, b, (((1,), (1,)), ((), ())), preferred_element_type=F32)


def dot_tn(a, b):
    return lax.dot_general(a, b, (((0,), (0,)), ((), ())), preferred_element_type=F32)


def kernel(
    sizes,
    vis_h,
    count_s,
    proj_h,
    text_h,
    gain_h,
    qw_h,
    qg_h,
    text_o,
    proj_o,
    qw,
    qi,
    qt,
    vis,
    txt,
    gain,
    ag,
    flat,
    wblk,
    ib,
    tb,
    gtxt,
    part,
    st,
    st_in,
    hs,
    hc,
    h1,
    hx,
    h2,
    hz,
    stage_t,
    stage_p,
    load_sem,
    out_sem,
    agz_s,
    agz_r,
    agx_s,
    agx_r,
    agc_s,
    agc_r,
    is_s,
    is_r,
    ts_s,
    ts_r,
    st_s,
    st_r,
    rc_s,
    rc_r,
    rx_s,
    rx_r,
    rz_s,
    rz_r,
):
    nz, nx, ny = sizes
    z = lax.axis_index("dp_0")
    x = lax.axis_index("dp_1")
    c = lax.axis_index("dp_2")
    y = lax.axis_index("mp")
    width = qw.shape[1]
    total = qw.shape[0]
    enc = vis.shape[1]
    text_rows = txt.shape[0]
    img_all = qi.shape[0]
    img_half = img_all // 2
    near = ny // 2
    slices = tb.shape[2]
    in_half = slices // 2
    tw = tb.shape[4]
    packed = width // LANES
    shard = proj_h.shape[0]
    live_shards = -(-enc * packed // shard)
    other = 1 - c

    def ring(i, n):
        return lax.rem(i, n)

    barrier = pltpu.get_barrier_semaphore()

    def greet(axis, me, n):
        def one(j, carry):
            pl.semaphore_signal(
                barrier, inc=1, device_id={axis: ring(me + j, n)}, device_id_type=MESH
            )
            return carry

        lax.fori_loop(1, n, one, 0)

    greet("mp", y, ny)
    greet("dp_1", x, nx)
    greet("dp_0", z, nz)
    pl.semaphore_signal(barrier, inc=1, device_id={"dp_2": other}, device_id_type=MESH)

    def load(src, dst, i):
        return pltpu.make_async_copy(src, dst, load_sem.at[i])

    rows_each = IMG + text_rows
    load(proj_h, ag.at[c, x, z], 0).start()
    load(qw_h, qw, 1).start()

    def rows_in(k):
        base = pl.multiple_of(k * rows_each, 16)
        to_i = qi.at[pl.ds(pl.multiple_of(k * IMG, 16), IMG)]
        return (
            load(qg_h.at[pl.ds(base, IMG)], to_i, 6 + k),
            load(
                qg_h.at[pl.ds(pl.multiple_of(base + IMG, 16), text_rows)],
                qt.at[k],
                6 + ny + k,
            ),
        )

    def start_rows(k, carry):
        a, b = rows_in(k)
        a.start()
        b.start()
        return carry

    lax.fori_loop(0, ny, start_rows, 0)
    load(vis_h, vis, 2).start()
    load(text_h, txt, 3).start()
    load(gain_h, gain, 4).start()

    def wait_rows(k, carry):
        a, b = rows_in(k)
        a.wait()
        b.wait()
        return carry

    lax.fori_loop(0, ny, wait_rows, 0)
    load(qw_h, qw, 1).wait()

    def owner_of(way, d):
        return ring(y + d, ny) if way == 0 else ring(y + ny - d, ny)

    def toward(way):
        return ring(y + 1, ny) if way == 0 else ring(y + ny - 1, ny)

    def img_dot(owner, h):
        rows = qi[pl.ds(pl.multiple_of(h * img_half, 16), img_half), :]
        block = qw[pl.ds(pl.multiple_of(owner * width, width), width), :]
        return dot_nt(rows, block)

    def img_send(way, d, h):
        return pltpu.make_async_remote_copy(
            src_ref=ib.at[way, d, h],
            dst_ref=ib.at[way, d - 1, h],
            send_sem=is_s.at[way, d - 1, h],
            recv_sem=is_r.at[way, d - 1, h],
            device_id={"mp": toward(way)},
            device_id_type=MESH,
        )

    def img_first(way, far):
        d = near if far else near - 1
        h = way if far else 1 - way
        ib[way, d, h] = img_dot(owner_of(way, d), h).astype(BF16)

    def img_first_send(way, far):
        d = near if far else near - 1
        h = way if far else 1 - way
        img_send(way, d, h).start()

    def relay_place(u, way):
        d = near - 1 - (u + 1) // 2
        h = lax.rem(u, 2) if way == 0 else 1 - lax.rem(u, 2)
        return d, h

    def img_relay(u, carry):
        for way in (0, 1):
            d, h = relay_place(u, way)
            mine = img_dot(owner_of(way, d), h)
            img_send(way, d + 1, h).wait_recv()
            ib[way, d, h] = (mine + ib[way, d, h].astype(F32)).astype(BF16)
            img_send(way, d, h).start()
        return carry

    for way in (0, 1):
        img_first(way, True)
    for way in (0, 1):
        img_first(way, False)

    load(proj_h, ag.at[c, x, z], 0).wait()
    pl.semaphore_wait(barrier, (ny - 1) + (nx - 1) + (nz - 1) + 1)

    for way in (0, 1):
        img_first_send(way, True)

    def agz(j):
        return pltpu.make_async_remote_copy(
            src_ref=ag.at[c, x, z],
            dst_ref=ag.at[c, x, z],
            send_sem=agz_s,
            recv_sem=agz_r,
            device_id={"dp_0": ring(z + j, nz)},
            device_id_type=MESH,
        )

    def agx(j):
        return pltpu.make_async_remote_copy(
            src_ref=ag.at[c, x],
            dst_ref=ag.at[c, x],
            send_sem=agx_s,
            recv_sem=agx_r,
            device_id={"dp_1": ring(x + j, nx)},
            device_id_type=MESH,
        )

    agc = pltpu.make_async_remote_copy(
        src_ref=ag.at[c],
        dst_ref=ag.at[c],
        send_sem=agc_s,
        recv_sem=agc_r,
        device_id={"dp_2": other},
        device_id_type=MESH,
    )

    def begin(make, n):
        def one(j, carry):
            make(j).start()
            return carry

        lax.fori_loop(1, n, one, 0)

    def drain(ref, sem):
        pltpu.make_async_copy(ref, ref, sem).wait()

    begin(agz, nz)
    for way in (0, 1):
        img_first_send(way, False)

    relays = ny - 3
    early = min(2, relays)
    lax.fori_loop(0, early, img_relay, 0)
    drain(ag.at[0, 0, pl.ds(0, nz - 1)], agz_r)
    begin(agx, nx)
    lax.fori_loop(early, relays, img_relay, 0)

    def text_dot(owner, s):
        cols = qw[pl.ds(pl.multiple_of(s * tw, tw), tw), :]
        return dot_nt(qt[owner], cols)

    def text_send(way, d, s):
        return pltpu.make_async_remote_copy(
            src_ref=tb.at[way, d, s],
            dst_ref=tb.at[way, d - 1, s],
            send_sem=ts_s.at[way, d - 1, s],
            recv_sem=ts_r.at[way, d - 1, s],
            device_id={"mp": toward(way)},
            device_id_type=MESH,
        )

    def text_first(i, carry):
        far = i < in_half
        k = lax.rem(i, in_half)
        d = jnp.where(far, near, near - 1)
        for way in (0, 1):
            h = jnp.where(far, way, 1 - way)
            s = h * in_half + k
            tb[way, d, s] = text_dot(owner_of(way, d), s).astype(BF16)
            text_send(way, d, s).start()
        return carry

    def text_relay(n, carry):
        u = n // in_half
        k = lax.rem(n, in_half)
        for way in (0, 1):
            d, h = relay_place(u, way)
            s = h * in_half + k
            mine = text_dot(owner_of(way, d), s)
            text_send(way, d + 1, s).wait_recv()
            tb[way, d, s] = (mine + tb[way, d, s].astype(F32)).astype(BF16)
            text_send(way, d, s).start()
        return carry

    lax.fori_loop(0, 2, text_first, 0)

    drain(ag.at[0, pl.ds(0, nx - 1)], agx_r)
    agc.start()

    own_sum = [img_dot(y, h) for h in (0, 1)]
    load(vis_h, vis, 2).wait()
    load(gain_h, gain, 4).wait()
    drain(ag.at[0], agc_r)

    def unpack(s, carry):
        zz, r = s // (2 * nx), lax.rem(s, 2 * nx)
        rows = pl.ds(pl.multiple_of(s * shard, 16), shard)
        flat[rows, :] = ag[lax.rem(r, 2), r // 2, zz].astype(F32)
        return carry

    lax.fori_loop(0, live_shards, unpack, 0)
    for q in range(packed):
        wblk[:, q * LANES : (q + 1) * LANES] = flat[pl.ds(q, enc, packed), :].astype(BF16)
    embed = jnp.dot(vis[...], wblk[...], preferred_element_type=F32).astype(BF16)
    embed = embed.astype(F32)

    sums = []
    for h in (0, 1):
        mine = own_sum[h]
        for way in (0, 1):
            img_send(way, 1, h).wait_recv()
            mine = mine + ib[way, 0, h].astype(F32)
        sums.append(mine)
    gain_block = gain[:, pl.ds(pl.multiple_of(y * width, LANES), width)]
    scaled = gain_block * jnp.concatenate(sums, axis=0)
    sq = jnp.sum(embed * embed, axis=1, keepdims=True)
    cross = jnp.sum(scaled * embed, axis=1, keepdims=True)
    lane = lax.broadcasted_iota(jnp.int32, (img_all, LANES), 1)
    both = jnp.where(lane == 0, sq, jnp.where(lane == 1, cross, 0.0))
    st[...] = both.T[:8, :]

    def st_send(j):
        return pltpu.make_async_remote_copy(
            src_ref=st,
            dst_ref=st_in.at[j - 1],
            send_sem=st_s,
            recv_sem=st_r,
            device_id={"mp": ring(y + j, ny)},
            device_id_type=MESH,
        )

    begin(st_send, ny)
    part[0:img_all, :] = scaled
    part[img_all : 2 * img_all, :] = embed
    lax.fori_loop(2, 2 * in_half, text_first, 0)

    drain(st_in, st_r)
    stats = st[...]
    for j in range(ny - 1):
        stats = stats + st_in[j]
    stats = jnp.concatenate([stats, jnp.zeros((LANES - 8, img_all), F32)], axis=0).T
    inv = lax.rsqrt(stats[:, 0:1] * (1.0 / total) + EPS)
    mean = stats[:, 1:2] * (1.0 / total)
    row = lax.broadcasted_iota(jnp.int32, (img_all, 1), 0)
    counts = jnp.zeros((img_all, 1), jnp.int32)
    for k in range(ny):
        counts = jnp.where(row // IMG == k, count_s[k], counts)
    live = lax.rem(row, IMG) // PATCH < counts
    grad = inv * part[0:img_all, :] - part[img_all : 2 * img_all, :] * (inv * inv * inv * mean)
    grad = jnp.where(live, grad, 0.0).astype(BF16)

    for q in range(packed):
        cols = dot_tn(vis[...], grad[:, q * LANES : (q + 1) * LANES])
        flat[pl.ds(q, enc, packed), :] = cols
    pad = flat.shape[0] - enc * packed
    if pad:
        flat[enc * packed :, :] = jnp.zeros((pad, LANES), F32)

    def pack(s, carry):
        zz, r = s // (2 * nx), lax.rem(s, 2 * nx)
        rows = pl.ds(pl.multiple_of(s * shard, 16), shard)
        hs[lax.rem(r, 2), r // 2, zz] = flat[rows, :].astype(BF16)
        return carry

    lax.fori_loop(0, 2 * nx * nz, pack, 0)
    rc = pltpu.make_async_remote_copy(
        src_ref=hs.at[other],
        dst_ref=hc,
        send_sem=rc_s,
        recv_sem=rc_r,
        device_id={"dp_2": other},
        device_id_type=MESH,
    )
    rc.start()

    def rx(j):
        return pltpu.make_async_remote_copy(
            src_ref=h1.at[ring(x + j, nx)],
            dst_ref=hx.at[j - 1],
            send_sem=rx_s,
            recv_sem=rx_r,
            device_id={"dp_1": ring(x + j, nx)},
            device_id_type=MESH,
        )

    def rz(j):
        return pltpu.make_async_remote_copy(
            src_ref=h2.at[ring(z + j, nz)],
            dst_ref=hz.at[j - 1],
            send_sem=rz_s,
            recv_sem=rz_r,
            device_id={"dp_0": ring(z + j, nz)},
            device_id_type=MESH,
        )

    steps = relays * in_half
    cut = [min(k, steps) for k in (2, 8, 14)]
    lax.fori_loop(0, cut[0], text_relay, 0)

    rc.wait_recv()

    def core_sum(s, carry):
        xx, zz = s // nz, lax.rem(s, nz)
        h1[xx, zz] = (hs[c, xx, zz].astype(F32) + hc[xx, zz].astype(F32)).astype(BF16)
        return carry

    lax.fori_loop(0, nx * nz, core_sum, 0)
    begin(rx, nx)
    lax.fori_loop(cut[0], cut[1], text_relay, 0)

    drain(hx, rx_r)

    def x_sum(zz, carry):
        acc = h1[x, zz].astype(F32)
        for j in range(nx - 1):
            acc = acc + hx[j, zz].astype(F32)
        h2[zz] = acc.astype(BF16)
        return carry

    lax.fori_loop(0, nz, x_sum, 0)
    begin(rz, nz)

    load(text_h, txt, 3).wait()
    sq_t = jnp.zeros((text_rows, 1), F32)
    for s in range(slices):
        rows_t = txt[:, s * tw : (s + 1) * tw].astype(F32)
        sq_t = sq_t + jnp.sum(rows_t * rows_t, axis=1, keepdims=True)
    lax.fori_loop(cut[1], cut[2], text_relay, 0)

    drain(hz, rz_r)
    acc = h2[z].astype(F32)
    for j in range(nz - 1):
        acc = acc + hz[j].astype(F32)
    stage_p[...] = acc * (float(nz * nx * 2 * img_all) ** -0.5)
    out_p = pltpu.make_async_copy(stage_p, proj_o, out_sem.at[0])
    out_p.start()
    lax.fori_loop(cut[2], steps, text_relay, 0)

    cross_t = jnp.zeros((text_rows, 1), F32)
    for k in range(in_half):
        for h in (1, 0):
            s = h * in_half + k
            g = text_dot(y, s)
            for way in (0, 1):
                text_send(way, 1, s).wait_recv()
                g = g + tb[way, 0, s].astype(F32)
            g = g * gain[:, s * tw : (s + 1) * tw]
            gtxt[s] = g
            rows_t = txt[:, s * tw : (s + 1) * tw].astype(F32)
            cross_t = cross_t + jnp.sum(g * rows_t, axis=1, keepdims=True)
    inv_t = lax.rsqrt(sq_t * (1.0 / total) + EPS)
    scale_t = inv_t * inv_t * inv_t * (cross_t * (1.0 / total))
    for s in range(slices):
        rows_t = txt[:, s * tw : (s + 1) * tw].astype(F32)
        stage_t[:, s * tw : (s + 1) * tw] = (inv_t * gtxt[s] - rows_t * scale_t).astype(BF16)
    out_t = pltpu.make_async_copy(stage_t, text_o, out_sem.at[1])
    out_t.start()

    drain(ag.at[0, 0, pl.ds(0, nz - 1)], agz_s)
    drain(ag.at[0, pl.ds(0, nx - 1)], agx_s)
    agc.wait_send()
    drain(st_in, st_s)
    rc.wait_send()
    drain(hx, rx_s)
    drain(hz, rz_s)
    for way in (0, 1):
        for d in range(1, near + 1):
            for h in (0, 1):
                if d < near or h == way:
                    img_send(way, d, h).wait_send()

                    def sent(k, carry, way=way, d=d, h=h):
                        text_send(way, d, h * in_half + k).wait_send()
                        return carry

                    lax.fori_loop(0, in_half, sent, 0)
    out_p.wait()
    out_t.wait()


def body(vision_rows, image_count, proj_flat, text_embeds, norm_gain, q_weight, q_grad):
    nz, nx, ny = (lax.axis_size(a) for a in ("dp_0", "dp_1", "mp"))
    total, width = q_weight.shape
    img_all, enc = vision_rows.shape
    text_rows = text_embeds.shape[0]
    shard = proj_flat.shape[0]
    near = ny // 2
    slices = 8
    tw = total // slices
    flat_rows = nz * nx * 2 * shard
    sem = pltpu.SemaphoreType.DMA
    any_space = pl.BlockSpec(memory_space=pl.ANY)
    scratch = [
        pltpu.VMEM((total, width), BF16),
        pltpu.VMEM((img_all, width), BF16),
        pltpu.VMEM((ny, text_rows, width), BF16),
        pltpu.VMEM((img_all, enc), BF16),
        pltpu.VMEM((text_rows, total), BF16),
        pltpu.VMEM((1, total), F32),
        pltpu.VMEM((2, nx, nz, shard, LANES), BF16),
        pltpu.VMEM((flat_rows, LANES), F32),
        pltpu.VMEM((enc, width), BF16),
        pltpu.VMEM((2, near + 1, 2, img_all // 2, width), BF16),
        pltpu.VMEM((2, near + 1, slices, text_rows, tw), BF16),
        pltpu.VMEM((slices, text_rows, tw), F32),
        pltpu.VMEM((2 * img_all, width), F32),
        pltpu.VMEM((8, img_all), F32),
        pltpu.VMEM((ny - 1, 8, img_all), F32),
        pltpu.VMEM((2, nx, nz, shard, LANES), BF16),
        pltpu.VMEM((nx, nz, shard, LANES), BF16),
        pltpu.VMEM((nx, nz, shard, LANES), BF16),
        pltpu.VMEM((nx - 1, nz, shard, LANES), BF16),
        pltpu.VMEM((nz, shard, LANES), BF16),
        pltpu.VMEM((nz - 1, shard, LANES), BF16),
        pltpu.VMEM((text_rows, total), BF16),
        pltpu.VMEM((shard, LANES), F32),
        sem((6 + 2 * ny,)),
        sem((2,)),
        *([sem] * 6),
        sem((2, near, 2)),
        sem((2, near, 2)),
        sem((2, near, slices)),
        sem((2, near, slices)),
        *([sem] * 8),
    ]
    return pl.pallas_call(
        functools.partial(kernel, (nz, nx, ny)),
        out_shape=(
            jax.ShapeDtypeStruct(text_embeds.shape, BF16),
            jax.ShapeDtypeStruct(proj_flat.shape, F32),
        ),
        in_specs=[
            any_space,
            pl.BlockSpec(memory_space=pltpu.SMEM),
            *([any_space] * 5),
        ],
        out_specs=(any_space, any_space),
        scratch_shapes=scratch,
        compiler_params=pltpu.CompilerParams(
            collective_id=0,
            has_side_effects=True,
            vmem_limit_bytes=56 * 1024 * 1024,
        ),
        name="step",
    )(vision_rows, image_count, proj_flat, text_embeds, norm_gain.reshape(1, -1), q_weight, q_grad)


def solution(mesh):
    finer = Mesh(mesh.devices.reshape(12, 4, 2, mesh.shape["mp"]), ("dp_0", "dp_1", "dp_2", "mp"))
    placed = (P(DP, None), P(DP), P(DP_MP, None), P(DP_MP, None), P(), P(None, "mp"), P(DP, "mp"))
    return jax.shard_map(
        body,
        mesh=finer,
        in_specs=placed,
        out_specs=(P(DP_MP, None), P(DP_MP, None)),
        check_vma=False,
    )
```

```python
import functools

import jax
import jax.numpy as jnp
from jax import lax
from jax.experimental import pallas as pl
from jax.experimental.pallas import tpu as pltpu
from jax.sharding import Mesh
from jax.sharding import PartitionSpec as P

IMG_MAX = 4
PATCH = 8
IMG = IMG_MAX * PATCH
LANES = 128
DP = ("dp_0", "dp_1", "dp_2")
DP_MP = ("dp_0", "dp_1", "dp_2", "mp")
EPS = 1e-05
MESH = pl.DeviceIdType.MESH
F32 = jnp.float32
BF16 = jnp.bfloat16


def dot_nt(a, b):
    return lax.dot_general(a, b, (((1,), (1,)), ((), ())), preferred_element_type=F32)


def kernel(
    sizes,
    vis_h,
    count_s,
    proj_h,
    text_h,
    gain_h,
    qw_h,
    qg_h,
    text_o,
    proj_o,
    qw,
    qi,
    qt,
    vis,
    vis_t,
    txt,
    gain,
    sy,
    rows_f,
    lhs,
    ag,
    flat,
    wblk,
    emb,
    tb,
    gtxt,
    st,
    st_in,
    hs,
    hc,
    h1,
    hx,
    h2,
    hz,
    ty,
    ty_in,
    load_sem,
    sy_s,
    sy_r,
    agz_s,
    agz_r,
    agx_s,
    agx_r,
    agc_s,
    agc_r,
    ts_s,
    ts_r,
    st_s,
    st_r,
    rc_s,
    rc_r,
    rx_s,
    rx_r,
    rz_s,
    rz_r,
    ty_s,
    ty_r,
):
    nz, nx, ny = sizes
    z = lax.axis_index("dp_0")
    x = lax.axis_index("dp_1")
    c = lax.axis_index("dp_2")
    y = lax.axis_index("mp")
    total, width = qw.shape
    enc = vis.shape[1]
    text_rows = txt.shape[0]
    img_all = qi.shape[0]
    near = ny // 2
    slices = tb.shape[2]
    in_half = slices // 2
    tw = tb.shape[4]
    packed = width // LANES
    shard = proj_h.shape[0]
    own_rows = lhs.shape[0]
    live_shards = -(-enc * packed // shard)
    other = 1 - c
    per_row = 1.0 / total

    def ring(i, n):
        return lax.rem(i, n)

    def drain(ref, sem):
        pltpu.make_async_copy(ref, ref, sem).wait()

    def begin(make, n):
        def one(j, carry):
            make(j).start()
            return carry

        lax.fori_loop(1, n, one, 0)

    def send(src, dst, send_sem, recv_sem, axis, index):
        return pltpu.make_async_remote_copy(
            src_ref=src,
            dst_ref=dst,
            send_sem=send_sem,
            recv_sem=recv_sem,
            device_id={axis: index},
            device_id_type=MESH,
        )

    barrier = pltpu.get_barrier_semaphore()

    def greet(axis, me, n):
        def one(j, carry):
            pl.semaphore_signal(
                barrier, inc=1, device_id={axis: ring(me + j, n)}, device_id_type=MESH
            )
            return carry

        lax.fori_loop(1, n, one, 0)

    greet("dp_0", z, nz)
    greet("mp", y, ny)
    greet("dp_1", x, nx)
    pl.semaphore_signal(barrier, inc=1, device_id={"dp_2": other}, device_id_type=MESH)

    def load(src, dst, i):
        return pltpu.make_async_copy(src, dst, load_sem.at[i])

    rows_each = IMG + text_rows

    def text_in(k):
        base = pl.multiple_of(k * rows_each + IMG, 16)
        return load(qg_h.at[pl.ds(base, text_rows)], qt.at[k], 6 + k)

    def img_in(k):
        base = pl.multiple_of(k * rows_each, 16)
        to = qi.at[pl.ds(pl.multiple_of(k * IMG, 16), IMG)]
        return load(qg_h.at[pl.ds(base, IMG)], to, 6 + ny + k)

    def start_all(make):
        def one(k, carry):
            make(k).start()
            return carry

        lax.fori_loop(0, ny, one, 0)

    def wait_all(make):
        def one(k, carry):
            make(k).wait()
            return carry

        lax.fori_loop(0, ny, one, 0)

    load(proj_h, ag.at[0, c, x, z], 0).start()
    load(proj_h, sy.at[y], 5).start()
    start_all(text_in)
    load(qw_h, qw, 1).start()
    load(gain_h, gain, 4).start()
    load(vis_h, vis, 2).start()
    start_all(img_in)
    load(text_h, txt, 3).start()
    rows_f[...] = jnp.zeros(rows_f.shape, F32)
    wait_all(text_in)
    load(qw_h, qw, 1).wait()

    def owner_of(way, d):
        return ring(y + d, ny) if way == 0 else ring(y + ny - d, ny)

    def text_dot(owner, s):
        cols = qw[pl.ds(pl.multiple_of(s * tw, tw), tw), :]
        return dot_nt(qt[owner], cols)

    def text_send(way, d, s):
        return send(
            tb.at[way, d, s],
            tb.at[way, d - 1, s],
            ts_s.at[way, d - 1, s],
            ts_r.at[way, d - 1, s],
            "mp",
            ring(y + 1, ny) if way == 0 else ring(y + ny - 1, ny),
        )

    def first_place(i, way):
        far = i < in_half
        h = jnp.where(far, way, 1 - way)
        return jnp.where(far, near, near - 1), h * in_half + lax.rem(i, in_half)

    def text_first(i, carry):
        for way in (0, 1):
            d, s = first_place(i, way)
            tb[way, d, s] = text_dot(owner_of(way, d), s).astype(BF16)
            text_send(way, d, s).start()
        return carry

    def relay_place(n, way):
        u = n // in_half
        h = lax.rem(u, 2) if way == 0 else 1 - lax.rem(u, 2)
        return near - 1 - (u + 1) // 2, h * in_half + lax.rem(n, in_half)

    def text_relay(n, carry):
        for way in (0, 1):
            d, s = relay_place(n, way)
            mine = text_dot(owner_of(way, d), s)
            text_send(way, d + 1, s).wait_recv()
            tb[way, d, s] = (mine + tb[way, d, s].astype(F32)).astype(BF16)
            text_send(way, d, s).start()
        return carry

    steps = (ny - 3) * in_half
    firsts = 2 * in_half
    done = [0, 0]

    def first(n):
        upto = min(done[0] + n, firsts)
        lax.fori_loop(done[0], upto, text_first, 0)
        done[0] = upto

    def relay(n):
        upto = min(done[1] + n, steps)
        lax.fori_loop(done[1], upto, text_relay, 0)
        done[1] = upto

    def agz(k):
        ref = ag.at[k, c, x, z]
        return lambda j: send(ref, ref, agz_s.at[k], agz_r.at[k], "dp_0", ring(z + j, nz))

    def agx(k):
        ref = ag.at[k, c, x]
        return lambda j: send(ref, ref, agx_s.at[k], agx_r.at[k], "dp_1", ring(x + j, nx))

    def agc(k):
        ref = ag.at[k, c]
        return send(ref, ref, agc_s.at[k], agc_r.at[k], "dp_2", other)

    def agz_wait(k, sem):
        drain(ag.at[0, 0, 0, pl.ds(0, nz - 1)], sem.at[k])

    def agx_wait(k, sem):
        drain(ag.at[0, 0, pl.ds(0, nx - 1)], sem.at[k])

    def agc_wait(k):
        drain(ag.at[0, 0], agc_r.at[k])

    def rc(k):
        return send(hs.at[k, other], hc.at[k], rc_s.at[k], rc_r.at[k], "dp_2", other)

    def rx(k):
        return lambda j: send(
            h1.at[k, ring(x + j, nx)],
            hx.at[k, j - 1],
            rx_s.at[k],
            rx_r.at[k],
            "dp_1",
            ring(x + j, nx),
        )

    def rz(k):
        return lambda j: send(
            h2.at[k, ring(z + j, nz)],
            hz.at[k, j - 1],
            rz_s.at[k],
            rz_r.at[k],
            "dp_0",
            ring(z + j, nz),
        )

    def st_send(k):
        return lambda j: send(
            st.at[k], st_in.at[k, j - 1], st_s.at[k], st_r.at[k], "mp", ring(y + j, ny)
        )

    def sy_send(j):
        return send(sy.at[y], sy.at[y], sy_s, sy_r, "mp", ring(y + j, ny))

    def ty_send(j):
        to = ring(y + j, ny)
        return send(ty.at[to], ty_in.at[j - 1], ty_s, ty_r, "mp", to)

    def unpack(k):
        def one(s, carry):
            zz, r = s // (2 * nx), lax.rem(s, 2 * nx)
            rows = pl.ds(pl.multiple_of(s * shard, 16), shard)
            flat[rows, :] = ag[k, lax.rem(r, 2), r // 2, zz].astype(F32)
            return carry

        lax.fori_loop(0, live_shards, one, 0)
        for q in range(packed):
            wblk[:, q * LANES : (q + 1) * LANES] = flat[pl.ds(q, enc, packed), :].astype(BF16)

    def pack(k, block):
        for q in range(packed):
            flat[pl.ds(q, enc, packed), :] = block[:, q * LANES : (q + 1) * LANES]
        pad = flat.shape[0] - enc * packed
        if pad:
            flat[enc * packed :, :] = jnp.zeros((pad, LANES), F32)

        def one(s, carry):
            zz, r = s // (2 * nx), lax.rem(s, 2 * nx)
            rows = pl.ds(pl.multiple_of(s * shard, 16), shard)
            hs[k, lax.rem(r, 2), r // 2, zz] = flat[rows, :].astype(BF16)
            return carry

        lax.fori_loop(0, 2 * nx * nz, one, 0)

    def core_sum(k):
        rc(k).wait_recv()

        def one(s, carry):
            xx, zz = s // nz, lax.rem(s, nz)
            pair = hs[k, c, xx, zz].astype(F32) + hc[k, xx, zz].astype(F32)
            h1[k, xx, zz] = pair.astype(BF16)
            return carry

        lax.fori_loop(0, nx * nz, one, 0)

    def x_sum(k):
        drain(hx.at[k], rx_r.at[k])

        def one(zz, carry):
            acc = h1[k, x, zz].astype(F32)
            for j in range(nx - 1):
                acc = acc + hx[k, j, zz].astype(F32)
            h2[k, zz] = acc.astype(BF16)
            return carry

        lax.fori_loop(0, nz, one, 0)

    def z_sum(k):
        drain(hz.at[k], rz_r.at[k])
        acc = h2[k, z].astype(F32)
        for j in range(nz - 1):
            acc = acc + hz[k, j].astype(F32)
        return acc

    def publish(k, column):
        wide = jnp.broadcast_to(column, (img_all, LANES))
        st[k] = wide.T[0:1, :]
        begin(st_send(k), ny)

    def collected(k):
        drain(st_in.at[k], st_r.at[k])
        row = st[k]
        for j in range(ny - 1):
            row = row + st_in[k, j]
        return jnp.broadcast_to(row, (LANES, img_all)).T[:, 0:1]

    for way in (0, 1):
        d, s = first_place(0, way)
        tb[way, d, s] = text_dot(owner_of(way, d), s).astype(BF16)
    done[0] = 1
    load(proj_h, ag.at[0, c, x, z], 0).wait()
    load(proj_h, sy.at[y], 5).wait()
    pl.semaphore_wait(barrier, (ny - 1) + (nx - 1) + (nz - 1) + 1)

    begin(sy_send, ny)
    begin(agz(0), nz)
    for way in (0, 1):
        d, s = first_place(0, way)
        text_send(way, d, s).start()
    first(2)

    load(gain_h, gain, 4).wait()
    drain(sy.at[pl.ds(0, ny - 1)], sy_r)
    for m in range(ny):
        rows_f[m, 0:shard, :] = sy[m].astype(F32)
        for q in range(packed):
            cols = slice(m * width + q * LANES, m * width + (q + 1) * LANES)
            piece = rows_f[m, pl.ds(q, own_rows, packed), :] * gain[:, cols]
            lhs[:, cols] = piece.astype(BF16)
    prod = jnp.dot(lhs[...], qw[...], preferred_element_type=F32)
    for q in range(packed):
        rows_f[0, pl.ds(q, own_rows, packed), :] = prod[:, q * LANES : (q + 1) * LANES]
    ag[1, c, x, z] = rows_f[0, 0:shard, :].astype(BF16)
    begin(agz(1), nz)

    first(1)
    load(vis_h, vis, 2).wait()
    vis_t[...] = vis[...].T
    agz_wait(0, agz_r)
    begin(agx(0), nx)
    first(firsts)
    relay(1)
    agz_wait(1, agz_r)
    begin(agx(1), nx)
    relay(1)
    agx_wait(0, agx_r)
    agc(0).start()
    relay(2)

    wait_all(img_in)
    agc_wait(0)
    unpack(0)
    embed = jnp.dot(vis[...], wblk[...], preferred_element_type=F32).astype(BF16)
    emb[...] = embed
    embed = embed.astype(F32)
    publish(0, jnp.sum(embed * embed, axis=1, keepdims=True))
    agx_wait(1, agx_r)
    agc(1).start()
    relay(2)

    row = lax.broadcasted_iota(jnp.int32, (img_all, 1), 0)
    counts = jnp.zeros((img_all, 1), jnp.int32)
    for k in range(ny):
        counts = jnp.where(row // IMG == k, count_s[k], counts)
    live = lax.rem(row, IMG) // PATCH < counts
    inv = lax.rsqrt(collected(0) * per_row + EPS)
    left = jnp.where(live, inv * qi[...].astype(F32), 0.0).astype(BF16)
    pack(0, jnp.dot(vis_t[...], left, preferred_element_type=F32))
    rc(0).start()

    agc_wait(1)
    unpack(1)
    back = jnp.dot(vis[...], wblk[...], preferred_element_type=F32)
    publish(1, jnp.sum(back * qi[...].astype(F32), axis=1, keepdims=True))
    relay(1)
    core_sum(0)
    begin(rx(0), nx)
    relay(1)
    mean = collected(1) * per_row
    right = jnp.where(live, (inv * inv * inv * mean) * emb[...].astype(F32), 0.0).astype(BF16)
    pack(1, jnp.dot(vis_t[...], right, preferred_element_type=F32))
    rc(1).start()
    relay(2)
    x_sum(0)
    begin(rz(0), nz)
    relay(1)
    core_sum(1)
    begin(rx(1), nx)

    load(text_h, txt, 3).wait()
    sq_t = jnp.zeros((text_rows, 1), F32)
    for s in range(slices):
        rows_t = txt[:, s * tw : (s + 1) * tw].astype(F32)
        sq_t = sq_t + jnp.sum(rows_t * rows_t, axis=1, keepdims=True)
    relay(3)
    x_sum(1)
    begin(rz(1), nz)
    relay(2)

    rows_f[0, 0:shard, :] = z_sum(0)
    for q in range(packed):
        lhs[:, q * LANES : (q + 1) * LANES] = rows_f[0, pl.ds(q, own_rows, packed), :].astype(BF16)
    term = lhs[:, 0:width]
    for m in range(ny):
        out = dot_nt(term, qw[m * width : (m + 1) * width, :])
        for q in range(packed):
            rows_f[m, pl.ds(q, own_rows, packed), :] = out[:, q * LANES : (q + 1) * LANES]
        ty[m] = rows_f[m, 0:shard, :].astype(BF16)
    begin(ty_send, ny)
    relay(steps)

    for k in range(in_half):
        for h in (0, 1):
            s = h * in_half + k
            g = text_dot(y, s)
            text_send(1 - h, 1, s).wait_recv()
            gtxt[s] = g + tb[1 - h, 0, s].astype(F32)

    second = z_sum(1)
    drain(ty_in, ty_r)
    one_term = ty[y].astype(F32)
    for j in range(ny - 1):
        one_term = one_term + ty_in[j].astype(F32)
    at = lax.rem(lax.broadcasted_iota(jnp.int32, (shard, LANES), 0), packed)
    gain_own = jnp.zeros((shard, LANES), F32)
    for q in range(packed):
        cols = pl.ds(pl.multiple_of(y * width + q * LANES, LANES), LANES)
        gain_own = jnp.where(at == q, gain[:, cols], gain_own)
    proj_o[...] = (gain_own * one_term - second) * (float(nz * nx * 2 * img_all) ** -0.5)

    cross_t = jnp.zeros((text_rows, 1), F32)
    for k in range(in_half):
        for h in (0, 1):
            s = h * in_half + k
            text_send(h, 1, s).wait_recv()
            g = (gtxt[s] + tb[h, 0, s].astype(F32)) * gain[:, s * tw : (s + 1) * tw]
            gtxt[s] = g
            rows_t = txt[:, s * tw : (s + 1) * tw].astype(F32)
            cross_t = cross_t + jnp.sum(g * rows_t, axis=1, keepdims=True)
    inv_t = lax.rsqrt(sq_t * per_row + EPS)
    scale_t = inv_t * inv_t * inv_t * (cross_t * per_row)
    for s in range(slices):
        cols = slice(s * tw, (s + 1) * tw)
        text_o[:, cols] = (inv_t * gtxt[s] - txt[:, cols].astype(F32) * scale_t).astype(BF16)

    drain(sy.at[pl.ds(0, ny - 1)], sy_s)
    for k in (0, 1):
        agz_wait(k, agz_s)
        agx_wait(k, agx_s)
        agc(k).wait_send()
        drain(st_in.at[k], st_s.at[k])
        rc(k).wait_send()
        drain(hx.at[k], rx_s.at[k])
        drain(hz.at[k], rz_s.at[k])
    drain(ty_in, ty_s)
    for way in (0, 1):
        for d in range(1, near + 1):
            for h in (0, 1):
                if d < near or h == way:

                    def sent(k, carry, way=way, d=d, h=h):
                        text_send(way, d, h * in_half + k).wait_send()
                        return carry

                    lax.fori_loop(0, in_half, sent, 0)


def put_out(text_v, proj_v, text_o, proj_o, sems):
    a = pltpu.make_async_copy(text_v, text_o, sems.at[0])
    b = pltpu.make_async_copy(proj_v, proj_o, sems.at[1])
    a.start()
    b.start()
    a.wait()
    b.wait()


def body(vision_rows, image_count, proj_flat, text_embeds, norm_gain, q_weight, q_grad):
    nz, nx, ny = (lax.axis_size(a) for a in ("dp_0", "dp_1", "mp"))
    total, width = q_weight.shape
    img_all, enc = vision_rows.shape
    text_rows = text_embeds.shape[0]
    shard = proj_flat.shape[0]
    packed = width // LANES
    own_rows = -(-shard // packed // 16) * 16
    near = ny // 2
    slices = 8
    tw = total // slices
    flat_rows = nz * nx * 2 * shard
    sem = pltpu.SemaphoreType.DMA
    any_space = pl.BlockSpec(memory_space=pl.ANY)
    in_vmem = pl.BlockSpec(memory_space=pltpu.VMEM)
    scratch = [
        pltpu.VMEM((total, width), BF16),
        pltpu.VMEM((img_all, width), BF16),
        pltpu.VMEM((ny, text_rows, width), BF16),
        pltpu.VMEM((img_all, enc), BF16),
        pltpu.VMEM((enc, img_all), BF16),
        pltpu.VMEM((text_rows, total), BF16),
        pltpu.VMEM((1, total), F32),
        pltpu.VMEM((ny, shard, LANES), BF16),
        pltpu.VMEM((ny, own_rows * packed, LANES), F32),
        pltpu.VMEM((own_rows, total), BF16),
        pltpu.VMEM((2, 2, nx, nz, shard, LANES), BF16),
        pltpu.VMEM((flat_rows, LANES), F32),
        pltpu.VMEM((enc, width), BF16),
        pltpu.VMEM((img_all, width), BF16),
        pltpu.VMEM((2, near + 1, slices, text_rows, tw), BF16),
        pltpu.VMEM((slices, text_rows, tw), F32),
        pltpu.VMEM((2, 1, img_all), F32),
        pltpu.VMEM((2, ny - 1, 1, img_all), F32),
        pltpu.VMEM((2, 2, nx, nz, shard, LANES), BF16),
        pltpu.VMEM((2, nx, nz, shard, LANES), BF16),
        pltpu.VMEM((2, nx, nz, shard, LANES), BF16),
        pltpu.VMEM((2, nx - 1, nz, shard, LANES), BF16),
        pltpu.VMEM((2, nz, shard, LANES), BF16),
        pltpu.VMEM((2, nz - 1, shard, LANES), BF16),
        pltpu.VMEM((ny, shard, LANES), BF16),
        pltpu.VMEM((ny - 1, shard, LANES), BF16),
        sem((6 + 2 * ny,)),
        sem,
        sem,
        *([sem((2,))] * 6),
        sem((2, near, slices)),
        sem((2, near, slices)),
        *([sem((2,))] * 8),
        sem,
        sem,
    ]
    text_v, proj_v = pl.pallas_call(
        functools.partial(kernel, (nz, nx, ny)),
        out_shape=(pltpu.VMEM(text_embeds.shape, BF16), pltpu.VMEM(proj_flat.shape, F32)),
        in_specs=[
            any_space,
            pl.BlockSpec(memory_space=pltpu.SMEM),
            *([any_space] * 5),
        ],
        out_specs=(in_vmem, in_vmem),
        scratch_shapes=scratch,
        compiler_params=pltpu.CompilerParams(
            collective_id=0,
            has_side_effects=True,
            vmem_limit_bytes=56 * 1024 * 1024,
        ),
        name="step",
    )(vision_rows, image_count, proj_flat, text_embeds, norm_gain.reshape(1, -1), q_weight, q_grad)
    return pl.pallas_call(
        put_out,
        out_shape=(
            jax.ShapeDtypeStruct(text_embeds.shape, BF16),
            jax.ShapeDtypeStruct(proj_flat.shape, F32),
        ),
        in_specs=[in_vmem] * 2,
        out_specs=(any_space, any_space),
        scratch_shapes=[sem((2,))],
        name="put_out",
    )(*(pltpu.with_memory_space_constraint(v, pltpu.VMEM) for v in (text_v, proj_v)))


def solution(mesh):
    finer = Mesh(mesh.devices.reshape(12, 4, 2, mesh.shape["mp"]), ("dp_0", "dp_1", "dp_2", "mp"))
    placed = (P(DP, None), P(DP), P(DP_MP, None), P(DP_MP, None), P(), P(None, "mp"), P(DP, "mp"))
    return jax.shard_map(
        body,
        mesh=finer,
        in_specs=placed,
        out_specs=(P(DP_MP, None), P(DP_MP, None)),
        check_vma=False,
    )
```

```python
import functools

import jax
import jax.numpy as jnp
from jax import lax
from jax.experimental import pallas as pl
from jax.experimental.pallas import tpu as pltpu
from jax.sharding import Mesh
from jax.sharding import PartitionSpec as P

IMG_MAX = 4
PATCH = 8
IMG = IMG_MAX * PATCH
LANES = 128
DP = ("dp_0", "dp_1", "dp_2")
DP_MP = ("dp_0", "dp_1", "dp_2", "mp")
EPS = 1e-05
LEAD = 5
EARLY = 5
MESH = pl.DeviceIdType.MESH
F32 = jnp.float32
BF16 = jnp.bfloat16


def dot_nt(a, b):
    return lax.dot_general(a, b, (((1,), (1,)), ((), ())), preferred_element_type=F32)


def kernel(
    sizes,
    vis_h,
    count_h,
    proj_h,
    text_h,
    gain_h,
    qw_h,
    qg_h,
    text_o,
    proj_o,
    qw,
    qi,
    qt,
    vis,
    vis_t,
    txt,
    gain,
    sy,
    rows_f,
    lhs,
    ag,
    flat,
    wblk,
    emb,
    tb,
    gtxt,
    cross_f,
    st,
    st_in,
    hs,
    hc,
    h1,
    hx,
    h2,
    hz,
    ty,
    ty_in,
    count_s,
    in_sem,
    y_sem,
    load_sem,
    sy_s,
    sy_r,
    agz_s,
    agz_r,
    agx_s,
    agx_r,
    agc_s,
    agc_r,
    ts_s,
    ts_r,
    st_s,
    st_r,
    rc_s,
    rc_r,
    rx_s,
    rx_r,
    rz_s,
    rz_r,
    ty_s,
    ty_r,
):
    nz, nx, ny = sizes
    z = lax.axis_index("dp_0")
    x = lax.axis_index("dp_1")
    c = lax.axis_index("dp_2")
    y = lax.axis_index("mp")
    total, width = qw.shape
    enc = vis.shape[1]
    text_rows = txt.shape[0]
    img_all = qi.shape[0]
    near = ny // 2
    slices = gtxt.shape[0]
    in_half = slices // 2
    tw = tb.shape[3]
    packed = width // LANES
    shard = proj_h.shape[0]
    own_rows = lhs.shape[0]
    live_z = hx.shape[2]
    other = 1 - c
    per_row = 1.0 / total

    def ring(i, n):
        return lax.rem(i, n)

    def drain(ref, sem):
        pltpu.make_async_copy(ref, ref, sem).wait()

    def begin(make, n):
        def one(i, carry):
            side = jnp.where(lax.rem(i, 2) == 1, (i + 1) // 2, -(i // 2))
            make(n // 2 + side).start()
            return carry

        lax.fori_loop(0, n - 1, one, 0)

    def send(src, dst, send_sem, recv_sem, axis, index):
        return pltpu.make_async_remote_copy(
            src_ref=src,
            dst_ref=dst,
            send_sem=send_sem,
            recv_sem=recv_sem,
            device_id={axis: index},
            device_id_type=MESH,
        )

    def load(src, dst, i):
        return pltpu.make_async_copy(src, dst, load_sem.at[i])

    rows_each = IMG + text_rows

    def text_in(k, i):
        base = pl.multiple_of(k * rows_each + IMG, 16)
        return load(qg_h.at[pl.ds(base, text_rows)], qt.at[k], i)

    def img_in(k):
        base = pl.multiple_of(k * rows_each, 16)
        to = qi.at[pl.ds(pl.multiple_of(k * IMG, 16), IMG)]
        return load(qg_h.at[pl.ds(base, IMG)], to, 7)

    def slice_in(s):
        cols = pl.ds(pl.multiple_of(s * tw, tw), tw)
        return load(qw_h.at[cols], qw.at[cols], 9 + lax.rem(s, in_half))

    def pair_wait(i):
        drain(qw.at[pl.ds(0, 2 * tw)], load_sem.at[9 + i])

    def each(n, act, lo=0):
        def one(k, carry):
            act(k)
            return carry

        lax.fori_loop(lo, n, one, 0)

    load(proj_h, ag.at[0, c, x, z], 0).start()
    load(proj_h, sy.at[y], 1).start()
    text_in(ring(y + near, ny), 5).start()
    slice_in(0).start()
    slice_in(in_half).start()

    barrier = pltpu.get_barrier_semaphore()

    def tell(what, axis, index):
        pl.semaphore_signal(what, inc=1, device_id={axis: index}, device_id_type=MESH)

    corner_z = ((x == 0) & (y == 0) & (c == 0)).astype(jnp.int32)
    corner_x = ((z == 0) & (y == 0) & (c == 0)).astype(jnp.int32)
    corner_y = ((z == 0) & (x == 0) & (c == 0)).astype(jnp.int32)
    rank_z = ring(z + nz - corner_z, nz)
    rank_x = ring(x + nx - corner_x, nx)

    def tell_z(what):
        return lambda r: tell(what, "dp_0", ring(r + corner_z, nz))

    def tell_x(what):
        return lambda r: tell(what, "dp_1", ring(r + corner_x, nx))

    def turn(v):
        return ring(jnp.where(v < near, v, ny + near - 1 - v) + ny - corner_y, ny)

    def awaits(a, b, j):
        return (turn(b) < turn(a)) | (j == 1) | (j == ny - 1)

    y_now = jnp.int32(0)
    for j in range(1, ny):
        v = ring(y + j, ny)
        y_now = y_now + awaits(y, v, j).astype(jnp.int32)

        @pl.when(awaits(v, y, j))
        def _(v=v):
            tell(barrier, "mp", v)

    each(nz, tell_z(barrier), rank_z + 1)
    each(nx, tell_x(barrier), rank_x + 1)

    @pl.when(c == 1)
    def _():
        tell(barrier, "dp_2", other)

    def next_slices(i):
        slice_in(i).start()
        slice_in(in_half + i).start()

    each(in_half, next_slices, 1)
    each(ny, lambda j: text_in(ring(y + near + j, ny), 6).start(), 1)
    load(gain_h, gain, 4).start()
    load(vis_h, vis, 2).start()
    each(ny, lambda k: img_in(k).start())
    load(text_h, txt, 3).start()
    load(count_h, count_s, 8).start()

    def owner_of(way, d):
        return ring(y + d, ny) if way == 0 else ring(y + ny - d, ny)

    def text_dot(owner, s):
        cols = qw[pl.ds(pl.multiple_of(s * tw, tw), tw), :]
        return dot_nt(qt[owner], cols)

    mid_sems = (near - 1) * slices // 2

    def arrival(way, d, h, k):
        mid = ((d - 1) * slices + h * in_half + k) // 2
        end = mid_sems + jnp.where(h == way, 1 + k, 0)
        return ts_r.at[way, jnp.where(d > 0, mid, end)]

    def text_send(way, d, h, k):
        s = h * in_half + k
        return send(
            tb.at[way, d * slices + s],
            tb.at[way, (d - 1) * slices + s],
            ts_s.at[way],
            arrival(way, d - 1, h, k),
            "mp",
            ring(y + 1, ny) if way == 0 else ring(y + ny - 1, ny),
        )

    def text_first(i):
        far = i < in_half
        k = lax.rem(i, in_half)
        for way in (0, 1):
            h = jnp.where(far, way, 1 - way)
            d = jnp.where(far, near, near - 1)
            s = h * in_half + k
            tb[way, d * slices + s] = text_dot(owner_of(way, d), s).astype(BF16)
            text_send(way, d, h, k).start()

    def text_next_first(i):
        @pl.when(i < in_half)
        def _():
            pair_wait(i)

        text_first(i)

    def text_relay(n):
        u = n // in_half
        k = lax.rem(n, in_half)
        d = near - 1 - (u + 1) // 2
        for way in (0, 1):
            h = lax.rem(u + way, 2)
            s = h * in_half + k
            slot = d * slices + s
            mine = text_dot(owner_of(way, d), s)

            @pl.when(lax.rem(k, 2) == 0)
            def _(way=way, d=d, h=h, k=k):
                drain(tb.at[way, pl.ds(0, 2)], arrival(way, d, h, k))

            tb[way, slot] = (mine + tb[way, slot].astype(F32)).astype(BF16)
            text_send(way, d, h, k).start()

    steps = (ny - 3) * in_half
    firsts = 2 * in_half
    pieces = firsts + steps
    ahead = jnp.maximum(LEAD - 3 * z // 4, 0) + jnp.maximum((5 - turn(y)) // 2, 0)
    out = [jnp.int32(1), 1]

    def pace(n, most=None, times=1, more=0):
        most = min(n + LEAD + 2 if most is None else most, pieces)
        upto = jnp.minimum(n + times * ahead + more, most)
        upto = jnp.maximum(upto, out[0])
        if out[1] < firsts:
            each(jnp.minimum(upto, firsts), text_next_first, jnp.minimum(out[0], firsts))
        if most > firsts:
            each(jnp.maximum(upto, firsts) - firsts, text_relay, jnp.maximum(out[0], firsts) - firsts)
        out[0], out[1] = upto, max(out[1], min(n, pieces))

    def text_near(k):
        @pl.when(k == 0)
        def _():
            for way in (0, 1):
                drain(tb.at[way, pl.ds(0, in_half)], arrival(way, 0, 1 - way, 0))

        for h in (0, 1):
            s = h * in_half + k
            gtxt[s] = text_dot(y, s) + tb[1 - h, s].astype(F32)

    def text_last(k):
        for h in (0, 1):
            s = h * in_half + k
            drain(tb.at[h, 0], arrival(h, 0, h, k))
            cols = pl.ds(pl.multiple_of(s * tw, LANES), tw)
            g = (gtxt[s] + tb[h, s].astype(F32)) * gain[:, cols]
            gtxt[s] = g
            prod = g * txt[:, cols].astype(F32)
            for q in range(tw // LANES):
                cross_f[...] += prod[:, q * LANES : (q + 1) * LANES]

    def agz(k):
        ref = ag.at[k, c, x, z]
        return lambda j: send(ref, ref, agz_s.at[k], agz_r.at[k], "dp_0", ring(z + j, nz))

    def agx(k):
        ref = ag.at[k, c, x, pl.ds(0, live_z)]
        return lambda j: send(ref, ref, agx_s.at[k], agx_r.at[k], "dp_1", ring(x + j, nx))

    def agc(k):
        ref = ag.at[k, c]
        return send(ref, ref, agc_s.at[k], agc_r.at[k], "dp_2", other)

    def agz_wait(k, sem):
        drain(ag.at[0, 0, 0, pl.ds(0, nz - 1)], sem.at[k])

    def agx_wait(k, sem):
        drain(ag.at[0, 0, pl.ds(0, nx - 1), pl.ds(0, live_z)], sem.at[k])

    def agc_wait(k):
        drain(ag.at[0, 0], agc_r.at[k])

    def rc(k):
        live = pl.ds(0, live_z)
        return send(
            hs.at[k, other, :, live], hc.at[k, :, live], rc_s.at[k], rc_r.at[k], "dp_2", other
        )

    def rx(k):
        return lambda j: send(
            h1.at[k, ring(x + j, nx), pl.ds(0, live_z)],
            hx.at[k, j - 1],
            rx_s.at[k],
            rx_r.at[k],
            "dp_1",
            ring(x + j, nx),
        )

    def rz(k):
        return lambda j: send(
            h2.at[k, ring(z + j, nz)],
            hz.at[k, j - 1],
            rz_s.at[k],
            rz_r.at[k],
            "dp_0",
            ring(z + j, nz),
        )

    def st_send(k):
        return lambda j: send(
            st.at[k], st_in.at[k, j - 1], st_s.at[k], st_r.at[k], "mp", ring(y + j, ny)
        )

    def sy_send(j):
        return send(sy.at[y], sy.at[y], sy_s, sy_r, "mp", ring(y + j, ny))

    def ty_send(j):
        to = ring(y + j, ny)
        return send(ty.at[to], ty_in.at[j - 1], ty_s, ty_r, "mp", to)

    def place(zz, r):
        return pl.ds(pl.multiple_of((zz * 2 * nx + r) * shard, 16), shard)

    def unpack(k):
        def one(zz):
            for r in range(2 * nx):
                flat[place(zz, r), :] = ag[k, r % 2, r // 2, zz].astype(F32)

        each(live_z, one)
        for q in range(packed):
            wblk[:, q * LANES : (q + 1) * LANES] = flat[pl.ds(q, enc, packed), :].astype(BF16)

    def pack(k, block):
        for q in range(packed):
            flat[pl.ds(q, enc, packed), :] = block[:, q * LANES : (q + 1) * LANES]
        end = live_z * 2 * nx * shard
        if end > enc * packed:
            flat[enc * packed : end, :] = jnp.zeros((end - enc * packed, LANES), F32)

        def one(zz):
            for r in range(2 * nx):
                hs[k, r % 2, r // 2, zz] = flat[place(zz, r), :].astype(BF16)

        each(live_z, one)

    def core_sum(k):
        rc(k).wait_recv()

        def one(zz):
            for xx in range(nx):
                pair = hs[k, c, xx, zz].astype(F32) + hc[k, xx, zz].astype(F32)
                h1[k, xx, zz] = pair.astype(BF16)

        each(live_z, one)

    def x_sum(k):
        drain(hx.at[k], rx_r.at[k])

        def one(zz):
            acc = h1[k, x, zz].astype(F32)
            for j in range(nx - 1):
                acc = acc + hx[k, j, zz].astype(F32)
            h2[k, zz] = acc.astype(BF16)

        each(live_z, one)

    def z_sum(k):
        drain(hz.at[k], rz_r.at[k])
        acc = h2[k, z].astype(F32)
        for j in range(nz - 1):
            acc = acc + hz[k, j].astype(F32)
        return acc

    def publish(k, column):
        wide = jnp.broadcast_to(column, (img_all, LANES))
        st[k] = wide.T[0:1, :]
        begin(st_send(k), ny)

    def collected(k):
        drain(st_in.at[k], st_r.at[k])
        row = st[k]
        for j in range(ny - 1):
            row = row + st_in[k, j]
        return jnp.broadcast_to(row, (LANES, img_all)).T[:, 0:1]

    pl.semaphore_wait(barrier, y_now + rank_z + rank_x + other)
    each(rank_z, tell_z(in_sem))
    each(rank_x, tell_x(in_sem))

    @pl.when(c == 0)
    def _():
        tell(in_sem, "dp_2", other)

    for j in range(1, ny):
        v = ring(y + j, ny)

        @pl.when(jnp.logical_not(awaits(v, y, j)))
        def _(v=v):
            tell(y_sem, "mp", v)

    pair_wait(0)
    text_in(ring(y + near, ny), 5).wait()
    text_first(jnp.int32(0))
    load(proj_h, sy.at[y], 1).wait()
    load(proj_h, ag.at[0, c, x, z], 0).wait()
    drain(qt.at[pl.ds(0, ny - 1)], load_sem.at[6])

    early = z < EARLY
    pace(1, 3, 0, (ny - 1 - turn(y)) // 3)

    @pl.when(y_now < ny - 1)
    def _():
        pl.semaphore_wait(y_sem, ny - 1 - y_now)

    begin(sy_send, ny)
    pace(1, firsts + 2, 2)
    rest = (nz - 1 - rank_z) + (nx - 1 - rank_x) + c

    @pl.when(rest > 0)
    def _():
        pl.semaphore_wait(in_sem, rest)

    begin(agz(0), nz)
    rows_f[...] = jnp.zeros(rows_f.shape, F32)
    cross_f[...] = jnp.zeros(cross_f.shape, F32)
    for k in (0, 1):
        h2[k, live_z:] = jnp.zeros((nz - live_z, shard, LANES), BF16)
    pace(4)
    load(vis_h, vis, 2).wait()
    vis_t[...] = vis[...].T
    pace(6)
    agz_wait(0, agz_r)
    begin(agx(0), nx)

    load(gain_h, gain, 4).wait()
    drain(sy.at[pl.ds(0, ny - 1)], sy_r)
    for m in range(ny):
        rows_f[m, 0:shard, :] = sy[m].astype(F32)
        for q in range(packed):
            cols = slice(m * width + q * LANES, m * width + (q + 1) * LANES)
            piece = rows_f[m, pl.ds(q, own_rows, packed), :] * gain[:, cols]
            lhs[:, cols] = piece.astype(BF16)
    prod = jnp.dot(lhs[...], qw[...], preferred_element_type=F32)
    for q in range(packed):
        rows_f[0, pl.ds(q, own_rows, packed), :] = prod[:, q * LANES : (q + 1) * LANES]
    ag[1, c, x, z] = rows_f[0, 0:shard, :].astype(BF16)
    begin(agz(1), nz)
    pace(9)
    agx_wait(0, agx_r)
    agc(0).start()

    drain(qi, load_sem.at[7])
    agz_wait(1, agz_r)
    begin(agx(1), nx)
    agc_wait(0)
    unpack(0)
    embed = jnp.dot(vis[...], wblk[...], preferred_element_type=F32).astype(BF16)
    emb[...] = embed
    embed = embed.astype(F32)
    publish(0, jnp.sum(embed * embed, axis=1, keepdims=True))
    pace(12)

    agx_wait(1, agx_r)
    agc(1).start()
    agc_wait(1)
    unpack(1)
    back = jnp.dot(vis[...], wblk[...], preferred_element_type=F32)
    publish(1, jnp.sum(back * qi[...].astype(F32), axis=1, keepdims=True))
    pace(14)

    load(count_h, count_s, 8).wait()
    row = lax.broadcasted_iota(jnp.int32, (img_all, 1), 0)
    counts = jnp.zeros((img_all, 1), jnp.int32)
    for k in range(ny):
        counts = jnp.where(row // IMG == k, count_s[k], counts)
    live = lax.rem(row, IMG) // PATCH < counts
    inv = lax.rsqrt(collected(0) * per_row + EPS)
    left = jnp.where(live, inv * qi[...].astype(F32), 0.0).astype(BF16)
    pack(0, jnp.dot(vis_t[...], left, preferred_element_type=F32))
    rc(0).start()
    pace(16)
    core_sum(0)
    begin(rx(0), nx)

    mean = collected(1) * per_row
    right = jnp.where(live, (inv * inv * inv * mean) * emb[...].astype(F32), 0.0).astype(BF16)
    pack(1, jnp.dot(vis_t[...], right, preferred_element_type=F32))
    rc(1).start()
    pace(18)
    core_sum(1)
    begin(rx(1), nx)
    pace(19)

    load(text_h, txt, 3).wait()
    sq_t = jnp.zeros((text_rows, 1), F32)
    for s in range(slices):
        rows_t = txt[:, s * tw : (s + 1) * tw].astype(F32)
        sq_t = sq_t + jnp.sum(rows_t * rows_t, axis=1, keepdims=True)
    x_sum(0)
    begin(rz(0), nz)
    pace(21)
    x_sum(1)
    begin(rz(1), nz)
    pace(23)

    rows_f[0, 0:shard, :] = z_sum(0)
    for q in range(packed):
        lhs[:, q * LANES : (q + 1) * LANES] = rows_f[0, pl.ds(q, own_rows, packed), :].astype(BF16)
    term = lhs[:, 0:width]
    for m in range(ny):
        prod = dot_nt(term, qw[m * width : (m + 1) * width, :])
        for q in range(packed):
            rows_f[m, pl.ds(q, own_rows, packed), :] = prod[:, q * LANES : (q + 1) * LANES]
        ty[m] = rows_f[m, 0:shard, :].astype(BF16)
    begin(ty_send, ny)
    pace(pieces)
    each(in_half, text_near)
    first_part = jnp.where(early, in_half, 0)
    each(first_part, text_last)
    second = z_sum(1)
    drain(ty_in, ty_r)
    one_term = ty[y].astype(F32)
    for j in range(ny - 1):
        one_term = one_term + ty_in[j].astype(F32)
    at = lax.rem(lax.broadcasted_iota(jnp.int32, (shard, LANES), 0), packed)
    gain_own = jnp.zeros((shard, LANES), F32)
    for q in range(packed):
        cols = pl.ds(pl.multiple_of(y * width + q * LANES, LANES), LANES)
        gain_own = jnp.where(at == q, gain[:, cols], gain_own)
    proj_o[...] = (gain_own * one_term - second) * (float(nz * nx * 2 * img_all) ** -0.5)
    each(in_half, text_last, first_part)

    cross_t = jnp.sum(cross_f[...], axis=1, keepdims=True)
    inv_t = lax.rsqrt(sq_t * per_row + EPS)
    scale_t = inv_t * inv_t * inv_t * (cross_t * per_row)
    for s in range(slices):
        cols = slice(s * tw, (s + 1) * tw)
        text_o[:, cols] = (inv_t * gtxt[s] - txt[:, cols].astype(F32) * scale_t).astype(BF16)

    drain(sy.at[pl.ds(0, ny - 1)], sy_s)
    for k in (0, 1):
        agz_wait(k, agz_s)
        agx_wait(k, agx_s)
        agc(k).wait_send()
        drain(st_in.at[k], st_s.at[k])
        rc(k).wait_send()
        drain(hx.at[k], rx_s.at[k])
        drain(hz.at[k], rz_s.at[k])
    drain(ty_in, ty_s)
    for way in (0, 1):
        drain(tb.at[way, pl.ds(0, pieces)], ts_s.at[way])


def put_out(text_v, proj_v, text_o, proj_o, sems):
    a = pltpu.make_async_copy(text_v, text_o, sems.at[0])
    b = pltpu.make_async_copy(proj_v, proj_o, sems.at[1])
    a.start()
    b.start()
    a.wait()
    b.wait()


def body(vision_rows, image_count, proj_flat, text_embeds, norm_gain, q_weight, q_grad):
    nz, nx, ny = (lax.axis_size(a) for a in ("dp_0", "dp_1", "mp"))
    total, width = q_weight.shape
    img_all, enc = vision_rows.shape
    text_rows = text_embeds.shape[0]
    shard = proj_flat.shape[0]
    packed = width // LANES
    own_rows = -(-shard // packed // 16) * 16
    near = ny // 2
    slices = 8
    tw = total // slices
    flat_rows = nz * nx * 2 * shard
    live_z = -(-enc * packed // (2 * nx * shard))
    sem = pltpu.SemaphoreType.DMA
    any_space = pl.BlockSpec(memory_space=pl.ANY)
    in_vmem = pl.BlockSpec(memory_space=pltpu.VMEM)
    scratch = [
        pltpu.VMEM((total, width), BF16),
        pltpu.VMEM((img_all, width), BF16),
        pltpu.VMEM((ny, text_rows, width), BF16),
        pltpu.VMEM((img_all, enc), BF16),
        pltpu.VMEM((enc, img_all), BF16),
        pltpu.VMEM((text_rows, total), BF16),
        pltpu.VMEM((1, total), F32),
        pltpu.VMEM((ny, shard, LANES), BF16),
        pltpu.VMEM((ny, own_rows * packed, LANES), F32),
        pltpu.VMEM((own_rows, total), BF16),
        pltpu.VMEM((2, 2, nx, nz, shard, LANES), BF16),
        pltpu.VMEM((flat_rows, LANES), F32),
        pltpu.VMEM((enc, width), BF16),
        pltpu.VMEM((img_all, width), BF16),
        pltpu.VMEM((2, (near + 1) * slices, text_rows, tw), BF16),
        pltpu.VMEM((slices, text_rows, tw), F32),
        pltpu.VMEM((text_rows, LANES), F32),
        pltpu.VMEM((2, 1, img_all), F32),
        pltpu.VMEM((2, ny - 1, 1, img_all), F32),
        pltpu.VMEM((2, 2, nx, nz, shard, LANES), BF16),
        pltpu.VMEM((2, nx, nz, shard, LANES), BF16),
        pltpu.VMEM((2, nx, nz, shard, LANES), BF16),
        pltpu.VMEM((2, nx - 1, live_z, shard, LANES), BF16),
        pltpu.VMEM((2, nz, shard, LANES), BF16),
        pltpu.VMEM((2, nz - 1, shard, LANES), BF16),
        pltpu.VMEM((ny, shard, LANES), BF16),
        pltpu.VMEM((ny - 1, shard, LANES), BF16),
        pltpu.SMEM((ny,), jnp.int32),
        pltpu.SemaphoreType.REGULAR,
        pltpu.SemaphoreType.REGULAR,
        sem((9 + slices // 2,)),
        sem,
        sem,
        *([sem((2,))] * 6),
        sem((2,)),
        sem((2, (near - 1) * slices // 2 + 1 + slices // 2)),
        *([sem((2,))] * 8),
        sem,
        sem,
    ]
    text_v, proj_v = pl.pallas_call(
        functools.partial(kernel, (nz, nx, ny)),
        out_shape=(pltpu.VMEM(text_embeds.shape, BF16), pltpu.VMEM(proj_flat.shape, F32)),
        in_specs=[any_space] * 7,
        out_specs=(in_vmem, in_vmem),
        scratch_shapes=scratch,
        compiler_params=pltpu.CompilerParams(
            collective_id=0,
            has_side_effects=True,
            vmem_limit_bytes=56 * 1024 * 1024,
        ),
        name="step",
    )(vision_rows, image_count, proj_flat, text_embeds, norm_gain.reshape(1, -1), q_weight, q_grad)
    return pl.pallas_call(
        put_out,
        out_shape=(
            jax.ShapeDtypeStruct(text_embeds.shape, BF16),
            jax.ShapeDtypeStruct(proj_flat.shape, F32),
        ),
        in_specs=[in_vmem] * 2,
        out_specs=(any_space, any_space),
        scratch_shapes=[sem((2,))],
        name="put_out",
    )(*(pltpu.with_memory_space_constraint(v, pltpu.VMEM) for v in (text_v, proj_v)))


def solution(mesh):
    finer = Mesh(mesh.devices.reshape(12, 4, 2, mesh.shape["mp"]), ("dp_0", "dp_1", "dp_2", "mp"))
    placed = (P(DP, None), P(DP), P(DP_MP, None), P(DP_MP, None), P(), P(None, "mp"), P(DP, "mp"))
    return jax.shard_map(
        body,
        mesh=finer,
        in_specs=placed,
        out_specs=(P(DP_MP, None), P(DP_MP, None)),
        check_vma=False,
    )
```

```python
import functools

import jax
import jax.numpy as jnp
from jax import lax
from jax.experimental import pallas as pl
from jax.experimental.pallas import tpu as pltpu
from jax.sharding import Mesh
from jax.sharding import PartitionSpec as P

IMG_MAX = 4
PATCH = 8
IMG = IMG_MAX * PATCH
LANES = 128
DP = ("dp_0", "dp_1", "dp_2")
DP_MP = ("dp_0", "dp_1", "dp_2", "mp")
EPS = 1e-05
LEAD = 5
EARLY = 5
MESH = pl.DeviceIdType.MESH
F32 = jnp.float32
BF16 = jnp.bfloat16


def dot_nt(a, b):
    return lax.dot_general(a, b, (((1,), (1,)), ((), ())), preferred_element_type=F32)


def kernel(
    sizes,
    vis_h,
    count_h,
    proj_h,
    text_h,
    gain_h,
    qw_h,
    qg_h,
    text_o,
    proj_o,
    qw,
    qi,
    qt,
    vis,
    vis_t,
    txt,
    gain,
    sy,
    rows_f,
    lhs,
    ag,
    flat,
    wblk,
    emb,
    tb,
    gtxt,
    cross_f,
    st,
    st_in,
    hs,
    hc,
    h1,
    hx,
    h2,
    hz,
    ty,
    ty_in,
    count_s,
    in_sem,
    y_sem,
    load_sem,
    sy_s,
    sy_r,
    agz_s,
    agz_r,
    agx_s,
    agx_r,
    agc_s,
    agc_r,
    ts_s,
    ts_r,
    st_s,
    st_r,
    rc_s,
    rc_r,
    rx_s,
    rx_r,
    rz_s,
    rz_r,
    ty_s,
    ty_r,
):
    nz, nx, ny = sizes
    z = lax.axis_index("dp_0")
    x = lax.axis_index("dp_1")
    c = lax.axis_index("dp_2")
    y = lax.axis_index("mp")
    total, width = qw.shape
    enc = vis.shape[1]
    text_rows = txt.shape[0]
    img_all = qi.shape[0]
    near = ny // 2
    slices = gtxt.shape[0]
    in_half = slices // 2
    tw = tb.shape[3]
    packed = width // LANES
    shard = proj_h.shape[0]
    own_rows = lhs.shape[0]
    live_z = -(-enc * packed // (2 * nx * shard))
    other = 1 - c
    per_row = 1.0 / total

    def ring(i, n):
        return lax.rem(i, n)

    def drain(ref, sem):
        pltpu.make_async_copy(ref, ref, sem).wait()

    def begin(make, n):
        def one(i, carry):
            side = jnp.where(lax.rem(i, 2) == 1, (i + 1) // 2, -(i // 2))
            make(n // 2 + side).start()
            return carry

        lax.fori_loop(0, n - 1, one, 0)

    def send(src, dst, send_sem, recv_sem, axis, index):
        return pltpu.make_async_remote_copy(
            src_ref=src,
            dst_ref=dst,
            send_sem=send_sem,
            recv_sem=recv_sem,
            device_id={axis: index},
            device_id_type=MESH,
        )

    def load(src, dst, i):
        return pltpu.make_async_copy(src, dst, load_sem.at[i])

    rows_each = IMG + text_rows

    def text_in(k, i):
        base = pl.multiple_of(k * rows_each + IMG, 16)
        return load(qg_h.at[pl.ds(base, text_rows)], qt.at[k], i)

    def img_in(k):
        base = pl.multiple_of(k * rows_each, 16)
        to = qi.at[pl.ds(pl.multiple_of(k * IMG, 16), IMG)]
        return load(qg_h.at[pl.ds(base, IMG)], to, 7)

    def slice_in(s):
        cols = pl.ds(pl.multiple_of(s * tw, tw), tw)
        return load(qw_h.at[cols], qw.at[cols], 9 + lax.rem(s, in_half))

    def pair_wait(i):
        drain(qw.at[pl.ds(0, 2 * tw)], load_sem.at[9 + i])

    def each(n, act, lo=0):
        def one(k, carry):
            act(k)
            return carry

        lax.fori_loop(lo, n, one, 0)

    load(proj_h, ag.at[0, c, x, z], 0).start()
    load(proj_h, sy.at[y], 1).start()
    text_in(ring(y + near, ny), 5).start()
    slice_in(0).start()
    slice_in(in_half).start()

    barrier = pltpu.get_barrier_semaphore()

    def tell(what, axis, index):
        pl.semaphore_signal(what, inc=1, device_id={axis: index}, device_id_type=MESH)

    corner_z = ((x == 0) & (y == 0) & (c == 0)).astype(jnp.int32)
    corner_x = ((z == 0) & (y == 0) & (c == 0)).astype(jnp.int32)
    corner_y = ((z == 0) & (x == 0) & (c == 0)).astype(jnp.int32)
    rank_z = ring(z + nz - corner_z, nz)
    rank_x = ring(x + nx - corner_x, nx)

    def tell_z(what):
        return lambda r: tell(what, "dp_0", ring(r + corner_z, nz))

    def tell_x(what):
        return lambda r: tell(what, "dp_1", ring(r + corner_x, nx))

    def turn(v):
        return ring(jnp.where(v < near, v, ny + near - 1 - v) + ny - corner_y, ny)

    def awaits(a, b, j):
        return (turn(b) < turn(a)) | (j == 1) | (j == ny - 1)

    y_now = jnp.int32(0)
    for j in range(1, ny):
        v = ring(y + j, ny)
        y_now = y_now + awaits(y, v, j).astype(jnp.int32)

        @pl.when(awaits(v, y, j))
        def _(v=v):
            tell(barrier, "mp", v)

    each(nz, tell_z(barrier), rank_z + 1)
    each(nx, tell_x(barrier), rank_x + 1)

    @pl.when(c == 1)
    def _():
        tell(barrier, "dp_2", other)

    def next_slices(i):
        slice_in(i).start()
        slice_in(in_half + i).start()

    each(in_half, next_slices, 1)
    each(ny, lambda j: text_in(ring(y + near + j, ny), 6).start(), 1)
    load(gain_h, gain, 4).start()
    load(vis_h, vis, 2).start()
    each(ny, lambda k: img_in(k).start())
    load(text_h, txt, 3).start()
    load(count_h, count_s, 8).start()

    def owner_of(way, d):
        return ring(y + d, ny) if way == 0 else ring(y + ny - d, ny)

    def text_dot(owner, s):
        cols = qw[pl.ds(pl.multiple_of(s * tw, tw), tw), :]
        return dot_nt(qt[owner], cols)

    mid_sems = (near - 1) * slices // 2

    def arrival(way, d, h, k):
        mid = ((d - 1) * slices + h * in_half + k) // 2
        end = mid_sems + jnp.where(h == way, 1 + k, 0)
        return ts_r.at[way, jnp.where(d > 0, mid, end)]

    def text_send(way, d, h, k):
        s = h * in_half + k
        return send(
            tb.at[way, d * slices + s],
            tb.at[way, (d - 1) * slices + s],
            ts_s.at[way],
            arrival(way, d - 1, h, k),
            "mp",
            ring(y + 1, ny) if way == 0 else ring(y + ny - 1, ny),
        )

    def text_first(i):
        far = i < in_half
        k = lax.rem(i, in_half)
        for way in (0, 1):
            h = jnp.where(far, way, 1 - way)
            d = jnp.where(far, near, near - 1)
            s = h * in_half + k
            tb[way, d * slices + s] = text_dot(owner_of(way, d), s).astype(BF16)
            text_send(way, d, h, k).start()

    def text_next_first(i):
        @pl.when(i < in_half)
        def _():
            pair_wait(i)

        text_first(i)

    def text_relay(n):
        u = n // in_half
        k = lax.rem(n, in_half)
        d = near - 1 - (u + 1) // 2
        for way in (0, 1):
            h = lax.rem(u + way, 2)
            s = h * in_half + k
            slot = d * slices + s
            mine = text_dot(owner_of(way, d), s)

            @pl.when(lax.rem(k, 2) == 0)
            def _(way=way, d=d, h=h, k=k):
                drain(tb.at[way, pl.ds(0, 2)], arrival(way, d, h, k))

            tb[way, slot] = (mine + tb[way, slot].astype(F32)).astype(BF16)
            text_send(way, d, h, k).start()

    steps = (ny - 3) * in_half
    firsts = 2 * in_half
    pieces = firsts + steps
    ahead = jnp.maximum(LEAD - 3 * z // 4, 0) + jnp.clip((6 - turn(y)) // 2, 0, 2)
    out = [jnp.int32(1), 1]

    def pace(n, most=None, times=1, more=0):
        most = min(n + LEAD + 2 if most is None else most, pieces)
        upto = jnp.minimum(n + times * ahead + more, most)
        upto = jnp.maximum(upto, out[0])
        if out[1] < firsts:
            each(jnp.minimum(upto, firsts), text_next_first, jnp.minimum(out[0], firsts))
        if most > firsts:
            each(jnp.maximum(upto, firsts) - firsts, text_relay, jnp.maximum(out[0], firsts) - firsts)
        out[0], out[1] = upto, max(out[1], min(n, pieces))

    def text_near(k):
        @pl.when(k == 0)
        def _():
            for way in (0, 1):
                drain(tb.at[way, pl.ds(0, in_half)], arrival(way, 0, 1 - way, 0))

        for h in (0, 1):
            s = h * in_half + k
            gtxt[s] = text_dot(y, s) + tb[1 - h, s].astype(F32)

    def text_last(k):
        for h in (0, 1):
            s = h * in_half + k
            drain(tb.at[h, 0], arrival(h, 0, h, k))
            cols = pl.ds(pl.multiple_of(s * tw, LANES), tw)
            g = (gtxt[s] + tb[h, s].astype(F32)) * gain[:, cols]
            gtxt[s] = g
            prod = g * txt[:, cols].astype(F32)
            for q in range(tw // LANES):
                cross_f[...] += prod[:, q * LANES : (q + 1) * LANES]

    def agz(k):
        ref = ag.at[k, c, x, z]
        return lambda j: send(ref, ref, agz_s.at[k], agz_r.at[k], "dp_0", ring(z + j, nz))

    def agx(k):
        ref = ag.at[k, c, x, pl.ds(0, live_z)]
        return lambda j: send(ref, ref, agx_s.at[k], agx_r.at[k], "dp_1", ring(x + j, nx))

    def agc(k):
        ref = ag.at[k, c]
        return send(ref, ref, agc_s.at[k], agc_r.at[k], "dp_2", other)

    def agz_wait(k, sem):
        drain(ag.at[0, 0, 0, pl.ds(0, nz - 1)], sem.at[k])

    def agx_wait(k, sem):
        drain(ag.at[0, 0, pl.ds(0, nx - 1), pl.ds(0, live_z)], sem.at[k])

    def agc_wait(k):
        drain(ag.at[0, 0], agc_r.at[k])

    def rc(k):
        live = pl.ds(0, live_z)
        return send(
            hs.at[k, other, :, live], hc.at[k, :, live], rc_s.at[k], rc_r.at[k], "dp_2", other
        )

    side_z = min(2, (nz - 1) // 2)
    near_z = 2 * side_z + 1
    runs = (pl.ds(near_z, nz - near_z), pl.ds(0, near_z))
    FAR, NEAR = 0, 1

    def slot_z(zz):
        return ring(zz - z + side_z + nz, nz)

    def rx(k, part):
        def one(j):
            to = ring(x + j, nx)
            src, dst = h1.at[k, to, runs[part]], hx.at[k, j - 1, runs[part]]
            return send(src, dst, rx_s.at[k], rx_r.at[k, part], "dp_1", to)

        begin(one, nx)

    def rz(k, part):
        def one(off):
            to = ring(z + off + nz, nz)
            return send(
                h2.at[k, off + side_z], hz.at[k, off + side_z], rz_s.at[k], rz_r.at[k], "dp_0", to
            )

        if part == NEAR:
            for off in range(side_z, 0, -1):
                one(off).start()
                one(-off).start()
            return

        def by_side(i):
            one(nz // 2 + jnp.where(lax.rem(i, 2) == 1, (i + 1) // 2, -(i // 2))).start()

        each(nz - near_z, by_side)

    def st_send(k):
        return lambda j: send(
            st.at[k], st_in.at[k, j - 1], st_s.at[k], st_r.at[k], "mp", ring(y + j, ny)
        )

    def sy_send(j):
        return send(sy.at[y], sy.at[y], sy_s, sy_r, "mp", ring(y + j, ny))

    def ty_send(j):
        to = ring(y + j, ny)
        return send(ty.at[to], ty_in.at[j - 1], ty_s, ty_r, "mp", to)

    def place(zz, r):
        return pl.ds(pl.multiple_of((zz * 2 * nx + r) * shard, 16), shard)

    def unpack(k):
        def one(zz):
            for r in range(2 * nx):
                flat[place(zz, r), :] = ag[k, r % 2, r // 2, zz].astype(F32)

        each(live_z, one)
        for q in range(packed):
            wblk[:, q * LANES : (q + 1) * LANES] = flat[pl.ds(q, enc, packed), :].astype(BF16)

    def pack(k, block):
        for q in range(packed):
            flat[pl.ds(q, enc, packed), :] = block[:, q * LANES : (q + 1) * LANES]
        end = live_z * 2 * nx * shard
        if end > enc * packed:
            flat[enc * packed : end, :] = jnp.zeros((end - enc * packed, LANES), F32)

        def one(zz):
            for r in range(2 * nx):
                hs[k, r % 2, r // 2, zz] = flat[place(zz, r), :].astype(BF16)

        each(live_z, one)

    def core_sum(k):
        rc(k).wait_recv()

        def one(zz):
            for xx in range(nx):
                pair = hs[k, c, xx, zz].astype(F32) + hc[k, xx, zz].astype(F32)
                h1[k, xx, slot_z(zz)] = pair.astype(BF16)

        each(live_z, one)

    def x_sum(k, part):
        drain(hx.at[k, :, runs[part]], rx_r.at[k, part])

        def one(slot):
            acc = h1[k, x, slot].astype(F32)
            for j in range(nx - 1):
                acc = acc + hx[k, j, slot].astype(F32)
            h2[k, slot] = acc.astype(BF16)

        lo, hi = (near_z, nz) if part == FAR else (0, near_z)
        each(hi, one, lo)
        rz(k, part)

    def z_sum(k):
        drain(hz.at[k, pl.ds(0, nz - 1)], rz_r.at[k])
        acc = h2[k, side_z].astype(F32)
        for slot in range(nz):
            if slot != side_z:
                acc = acc + hz[k, slot].astype(F32)
        return acc

    def publish(k, column):
        wide = jnp.broadcast_to(column, (img_all, LANES))
        st[k] = wide.T[0:1, :]
        begin(st_send(k), ny)

    def collected(k):
        drain(st_in.at[k], st_r.at[k])
        row = st[k]
        for j in range(ny - 1):
            row = row + st_in[k, j]
        return jnp.broadcast_to(row, (LANES, img_all)).T[:, 0:1]

    pl.semaphore_wait(barrier, y_now + rank_z + rank_x + other)
    each(rank_z, tell_z(in_sem))
    each(rank_x, tell_x(in_sem))

    @pl.when(c == 0)
    def _():
        tell(in_sem, "dp_2", other)

    for j in range(1, ny):
        v = ring(y + j, ny)

        @pl.when(jnp.logical_not(awaits(v, y, j)))
        def _(v=v):
            tell(y_sem, "mp", v)

    pair_wait(0)
    text_in(ring(y + near, ny), 5).wait()
    text_first(jnp.int32(0))
    load(proj_h, sy.at[y], 1).wait()
    load(proj_h, ag.at[0, c, x, z], 0).wait()
    drain(qt.at[pl.ds(0, ny - 1)], load_sem.at[6])

    early = z < EARLY
    pace(1, 3, 0, (ny - 1 - turn(y)) // 3)

    @pl.when(y_now < ny - 1)
    def _():
        pl.semaphore_wait(y_sem, ny - 1 - y_now)

    begin(sy_send, ny)
    pace(1, firsts + 2, 2)
    rest = (nz - 1 - rank_z) + (nx - 1 - rank_x) + c

    @pl.when(rest > 0)
    def _():
        pl.semaphore_wait(in_sem, rest)

    begin(agz(0), nz)
    rows_f[...] = jnp.zeros(rows_f.shape, F32)
    cross_f[...] = jnp.zeros(cross_f.shape, F32)
    for k in (0, 1):
        for zz in range(live_z, nz):
            h1[k, :, slot_z(zz)] = jnp.zeros((nx, shard, LANES), BF16)
    pace(4)
    load(vis_h, vis, 2).wait()
    vis_t[...] = vis[...].T
    pace(6)
    agz_wait(0, agz_r)
    begin(agx(0), nx)

    load(gain_h, gain, 4).wait()
    drain(sy.at[pl.ds(0, ny - 1)], sy_r)
    for m in range(ny):
        rows_f[m, 0:shard, :] = sy[m].astype(F32)
        for q in range(packed):
            cols = slice(m * width + q * LANES, m * width + (q + 1) * LANES)
            piece = rows_f[m, pl.ds(q, own_rows, packed), :] * gain[:, cols]
            lhs[:, cols] = piece.astype(BF16)
    prod = jnp.dot(lhs[...], qw[...], preferred_element_type=F32)
    for q in range(packed):
        rows_f[0, pl.ds(q, own_rows, packed), :] = prod[:, q * LANES : (q + 1) * LANES]
    ag[1, c, x, z] = rows_f[0, 0:shard, :].astype(BF16)
    begin(agz(1), nz)
    pace(9)
    agx_wait(0, agx_r)
    agc(0).start()

    drain(qi, load_sem.at[7])
    agz_wait(1, agz_r)
    begin(agx(1), nx)
    agc_wait(0)
    unpack(0)
    embed = jnp.dot(vis[...], wblk[...], preferred_element_type=F32).astype(BF16)
    emb[...] = embed
    embed = embed.astype(F32)
    publish(0, jnp.sum(embed * embed, axis=1, keepdims=True))
    pace(13)

    agx_wait(1, agx_r)
    agc(1).start()
    agc_wait(1)
    unpack(1)
    back = jnp.dot(vis[...], wblk[...], preferred_element_type=F32)
    publish(1, jnp.sum(back * qi[...].astype(F32), axis=1, keepdims=True))
    pace(14)

    load(count_h, count_s, 8).wait()
    row = lax.broadcasted_iota(jnp.int32, (img_all, 1), 0)
    counts = jnp.zeros((img_all, 1), jnp.int32)
    for k in range(ny):
        counts = jnp.where(row // IMG == k, count_s[k], counts)
    live = lax.rem(row, IMG) // PATCH < counts
    inv = lax.rsqrt(collected(0) * per_row + EPS)
    left = jnp.where(live, inv * qi[...].astype(F32), 0.0).astype(BF16)
    pack(0, jnp.dot(vis_t[...], left, preferred_element_type=F32))
    rc(0).start()
    pace(16)
    core_sum(0)
    rx(0, FAR)
    rx(0, NEAR)
    pace(17)

    mean = collected(1) * per_row
    right = jnp.where(live, (inv * inv * inv * mean) * emb[...].astype(F32), 0.0).astype(BF16)
    pack(1, jnp.dot(vis_t[...], right, preferred_element_type=F32))
    rc(1).start()
    pace(19)
    core_sum(1)
    rx(1, FAR)
    rx(1, NEAR)
    x_sum(0, FAR)
    pace(20)

    load(text_h, txt, 3).wait()
    sq_t = jnp.zeros((text_rows, 1), F32)
    for s in range(slices):
        rows_t = txt[:, s * tw : (s + 1) * tw].astype(F32)
        sq_t = sq_t + jnp.sum(rows_t * rows_t, axis=1, keepdims=True)
    x_sum(0, NEAR)
    pace(22)
    x_sum(1, FAR)
    pace(24, pieces - 2)

    rows_f[0, 0:shard, :] = z_sum(0)
    for q in range(packed):
        lhs[:, q * LANES : (q + 1) * LANES] = rows_f[0, pl.ds(q, own_rows, packed), :].astype(BF16)
    term = lhs[:, 0:width]
    for m in range(ny):
        prod = dot_nt(term, qw[m * width : (m + 1) * width, :])
        for q in range(packed):
            rows_f[m, pl.ds(q, own_rows, packed), :] = prod[:, q * LANES : (q + 1) * LANES]
        ty[m] = rows_f[m, 0:shard, :].astype(BF16)
    begin(ty_send, ny)
    x_sum(1, NEAR)
    pace(pieces)
    each(in_half, text_near)
    first_part = jnp.where(early, in_half, 0)
    each(first_part, text_last)
    second = z_sum(1)
    drain(ty_in, ty_r)
    one_term = ty[y].astype(F32)
    for j in range(ny - 1):
        one_term = one_term + ty_in[j].astype(F32)
    at = lax.rem(lax.broadcasted_iota(jnp.int32, (shard, LANES), 0), packed)
    gain_own = jnp.zeros((shard, LANES), F32)
    for q in range(packed):
        cols = pl.ds(pl.multiple_of(y * width + q * LANES, LANES), LANES)
        gain_own = jnp.where(at == q, gain[:, cols], gain_own)
    proj_o[...] = (gain_own * one_term - second) * (float(nz * nx * 2 * img_all) ** -0.5)
    each(in_half, text_last, first_part)

    cross_t = jnp.sum(cross_f[...], axis=1, keepdims=True)
    inv_t = lax.rsqrt(sq_t * per_row + EPS)
    scale_t = inv_t * inv_t * inv_t * (cross_t * per_row)
    for s in range(slices):
        cols = slice(s * tw, (s + 1) * tw)
        text_o[:, cols] = (inv_t * gtxt[s] - txt[:, cols].astype(F32) * scale_t).astype(BF16)

    drain(sy.at[pl.ds(0, ny - 1)], sy_s)
    for k in (0, 1):
        agz_wait(k, agz_s)
        agx_wait(k, agx_s)
        agc(k).wait_send()
        drain(st_in.at[k], st_s.at[k])
        rc(k).wait_send()
        drain(hx.at[k], rx_s.at[k])
        drain(hz.at[k, pl.ds(0, nz - 1)], rz_s.at[k])
    drain(ty_in, ty_s)
    for way in (0, 1):
        drain(tb.at[way, pl.ds(0, pieces)], ts_s.at[way])


def put_out(text_v, proj_v, text_o, proj_o, sems):
    a = pltpu.make_async_copy(text_v, text_o, sems.at[0])
    b = pltpu.make_async_copy(proj_v, proj_o, sems.at[1])
    a.start()
    b.start()
    a.wait()
    b.wait()


def body(vision_rows, image_count, proj_flat, text_embeds, norm_gain, q_weight, q_grad):
    nz, nx, ny = (lax.axis_size(a) for a in ("dp_0", "dp_1", "mp"))
    total, width = q_weight.shape
    img_all, enc = vision_rows.shape
    text_rows = text_embeds.shape[0]
    shard = proj_flat.shape[0]
    packed = width // LANES
    own_rows = -(-shard // packed // 16) * 16
    near = ny // 2
    slices = 8
    tw = total // slices
    flat_rows = nz * nx * 2 * shard
    sem = pltpu.SemaphoreType.DMA
    any_space = pl.BlockSpec(memory_space=pl.ANY)
    in_vmem = pl.BlockSpec(memory_space=pltpu.VMEM)
    scratch = [
        pltpu.VMEM((total, width), BF16),
        pltpu.VMEM((img_all, width), BF16),
        pltpu.VMEM((ny, text_rows, width), BF16),
        pltpu.VMEM((img_all, enc), BF16),
        pltpu.VMEM((enc, img_all), BF16),
        pltpu.VMEM((text_rows, total), BF16),
        pltpu.VMEM((1, total), F32),
        pltpu.VMEM((ny, shard, LANES), BF16),
        pltpu.VMEM((ny, own_rows * packed, LANES), F32),
        pltpu.VMEM((own_rows, total), BF16),
        pltpu.VMEM((2, 2, nx, nz, shard, LANES), BF16),
        pltpu.VMEM((flat_rows, LANES), F32),
        pltpu.VMEM((enc, width), BF16),
        pltpu.VMEM((img_all, width), BF16),
        pltpu.VMEM((2, (near + 1) * slices, text_rows, tw), BF16),
        pltpu.VMEM((slices, text_rows, tw), F32),
        pltpu.VMEM((text_rows, LANES), F32),
        pltpu.VMEM((2, 1, img_all), F32),
        pltpu.VMEM((2, ny - 1, 1, img_all), F32),
        pltpu.VMEM((2, 2, nx, nz, shard, LANES), BF16),
        pltpu.VMEM((2, nx, nz, shard, LANES), BF16),
        pltpu.VMEM((2, nx, nz, shard, LANES), BF16),
        pltpu.VMEM((2, nx - 1, nz, shard, LANES), BF16),
        pltpu.VMEM((2, nz, shard, LANES), BF16),
        pltpu.VMEM((2, nz, shard, LANES), BF16),
        pltpu.VMEM((ny, shard, LANES), BF16),
        pltpu.VMEM((ny - 1, shard, LANES), BF16),
        pltpu.SMEM((ny,), jnp.int32),
        pltpu.SemaphoreType.REGULAR,
        pltpu.SemaphoreType.REGULAR,
        sem((9 + slices // 2,)),
        sem,
        sem,
        *([sem((2,))] * 6),
        sem((2,)),
        sem((2, (near - 1) * slices // 2 + 1 + slices // 2)),
        *([sem((2,))] * 5),
        sem((2, 2)),
        *([sem((2,))] * 2),
        sem,
        sem,
    ]
    text_v, proj_v = pl.pallas_call(
        functools.partial(kernel, (nz, nx, ny)),
        out_shape=(pltpu.VMEM(text_embeds.shape, BF16), pltpu.VMEM(proj_flat.shape, F32)),
        in_specs=[any_space] * 7,
        out_specs=(in_vmem, in_vmem),
        scratch_shapes=scratch,
        compiler_params=pltpu.CompilerParams(
            collective_id=0,
            has_side_effects=True,
            vmem_limit_bytes=56 * 1024 * 1024,
        ),
        name="step",
    )(vision_rows, image_count, proj_flat, text_embeds, norm_gain.reshape(1, -1), q_weight, q_grad)
    return pl.pallas_call(
        put_out,
        out_shape=(
            jax.ShapeDtypeStruct(text_embeds.shape, BF16),
            jax.ShapeDtypeStruct(proj_flat.shape, F32),
        ),
        in_specs=[in_vmem] * 2,
        out_specs=(any_space, any_space),
        scratch_shapes=[sem((2,))],
        name="put_out",
    )(*(pltpu.with_memory_space_constraint(v, pltpu.VMEM) for v in (text_v, proj_v)))


def solution(mesh):
    finer = Mesh(mesh.devices.reshape(12, 4, 2, mesh.shape["mp"]), ("dp_0", "dp_1", "dp_2", "mp"))
    placed = (P(DP, None), P(DP), P(DP_MP, None), P(DP_MP, None), P(), P(None, "mp"), P(DP, "mp"))
    return jax.shard_map(
        body,
        mesh=finer,
        in_specs=placed,
        out_specs=(P(DP_MP, None), P(DP_MP, None)),
        check_vma=False,
    )
```

```python
import functools

import jax
import jax.numpy as jnp
from jax import lax
from jax.experimental import pallas as pl
from jax.experimental.pallas import tpu as pltpu
from jax.sharding import Mesh
from jax.sharding import PartitionSpec as P

IMG_MAX = 4
PATCH = 8
IMG = IMG_MAX * PATCH
LANES = 128
DP = ("dp_0", "dp_1", "dp_2")
DP_MP = ("dp_0", "dp_1", "dp_2", "mp")
EPS = 1e-05
LEAD = 7
SLACK = 143
EARLY = 3
MESH = pl.DeviceIdType.MESH
F32 = jnp.float32
BF16 = jnp.bfloat16


def dot_nt(a, b):
    return lax.dot_general(a, b, (((1,), (1,)), ((), ())), preferred_element_type=F32)


def kernel(
    sizes,
    vis_h,
    count_h,
    proj_h,
    text_h,
    gain_h,
    qw_h,
    qg_h,
    text_o,
    proj_o,
    qw,
    qi,
    qt,
    vis,
    vis_t,
    txt,
    gain,
    sy,
    rows_f,
    lhs,
    ag,
    flat,
    wblk,
    emb,
    tb,
    gtxt,
    cross_f,
    sq_f,
    st,
    st_in,
    hs,
    hc,
    h1,
    hx,
    h2,
    hz,
    ty,
    ty_in,
    count_s,
    ts_s,
    ts_r,
):
    nz, nx, ny = sizes
    text_rows, total = txt.shape
    near = ny // 2
    slices = gtxt.shape[0]
    in_half = slices // 2
    tw = tb.shape[3]
    per_row = 1.0 / total
    pieces = 2 * in_half + (ny - 3) * in_half
    mid_sems = (near - 1) * slices // 2

    def drain(ref, sem):
        pltpu.make_async_copy(ref, ref, sem).wait()

    def each(n, act, lo=0):
        def one(k, carry):
            act(k)
            return carry

        lax.fori_loop(lo, n, one, 0)

    def arrival(way, d, h, k):
        mid = ((d - 1) * slices + h * in_half + k) // 2
        end = mid_sems + jnp.where(h == way, 1 + k, 0)
        return ts_r.at[way, jnp.where(d > 0, mid, end)]

    def text_last(k):
        for h in (0, 1):
            s = h * in_half + k
            drain(tb.at[h, 0], arrival(h, 0, h, k))
            cols = pl.ds(pl.multiple_of(s * tw, LANES), tw)
            g = (gtxt[s] + tb[h, s].astype(F32)) * gain[:, cols]
            gtxt[s] = g
            prod = g * txt[:, cols].astype(F32)
            for q in range(tw // LANES):
                cross_f[...] += prod[:, q * LANES : (q + 1) * LANES]

    def work(
        in_sem,
        y_sem,
        load_sem,
        sy_s,
        sy_r,
        agz_s,
        agz_r,
        agx_s,
        agx_r,
        agc_s,
        agc_r,
        st_s,
        st_r,
        rc_s,
        rc_r,
        rx_s,
        rx_r,
        rz_s,
        rz_r,
        ty_s,
        ty_r,
    ):
        z = lax.axis_index("dp_0")
        x = lax.axis_index("dp_1")
        c = lax.axis_index("dp_2")
        y = lax.axis_index("mp")
        width = qw.shape[1]
        enc = vis.shape[1]
        img_all = qi.shape[0]
        packed = width // LANES
        shard = proj_h.shape[0]
        own_rows = lhs.shape[0]
        live_z = -(-enc * packed // (2 * nx * shard))
        other = 1 - c

        def ring(i, n):
            return lax.rem(i, n)

        def begin(make, n):
            def one(i, carry):
                side = jnp.where(lax.rem(i, 2) == 1, (i + 1) // 2, -(i // 2))
                make(n // 2 + side).start()
                return carry

            lax.fori_loop(0, n - 1, one, 0)

        def send(src, dst, send_sem, recv_sem, axis, index):
            return pltpu.make_async_remote_copy(
                src_ref=src,
                dst_ref=dst,
                send_sem=send_sem,
                recv_sem=recv_sem,
                device_id={axis: index},
                device_id_type=MESH,
            )

        def load(src, dst, i):
            return pltpu.make_async_copy(src, dst, load_sem.at[i])

        rows_each = IMG + text_rows

        def text_in(k, i):
            base = pl.multiple_of(k * rows_each + IMG, 16)
            return load(qg_h.at[pl.ds(base, text_rows)], qt.at[k], i)

        def img_in(k):
            base = pl.multiple_of(k * rows_each, 16)
            to = qi.at[pl.ds(pl.multiple_of(k * IMG, 16), IMG)]
            return load(qg_h.at[pl.ds(base, IMG)], to, 7)

        def slice_in(s):
            cols = pl.ds(pl.multiple_of(s * tw, tw), tw)
            return load(qw_h.at[cols], qw.at[cols], 9 + lax.rem(s, in_half))

        def pair_wait(i):
            drain(qw.at[pl.ds(0, 2 * tw)], load_sem.at[9 + i])

        slice_in(0).start()
        text_in(ring(y + near, ny), 5).start()
        slice_in(in_half).start()
        load(proj_h, ag.at[0, c, x, z], 0).start()
        load(proj_h, sy.at[y], 1).start()

        barrier = pltpu.get_barrier_semaphore()

        def tell(what, axis, index):
            pl.semaphore_signal(what, inc=1, device_id={axis: index}, device_id_type=MESH)

        corner_z = ((x == 0) & (y == 0) & (c == 0)).astype(jnp.int32)
        corner_x = ((z == 0) & (y == 0) & (c == 0)).astype(jnp.int32)
        corner_y = ((z == 0) & (x == 0) & (c == 0)).astype(jnp.int32)
        rank_z = ring(z + nz - corner_z, nz)
        rank_x = ring(x + nx - corner_x, nx)

        def tell_z(what):
            return lambda r: tell(what, "dp_0", ring(r + corner_z, nz))

        def tell_x(what):
            return lambda r: tell(what, "dp_1", ring(r + corner_x, nx))

        def turn(v):
            place = jnp.where(v < near, v, ny + near - 1 - v)
            place = jnp.where(place == near, near - 1, jnp.where(place == near - 1, near, place))
            return ring(place + ny - corner_y, ny)

        def awaits(a, b, j):
            return (turn(b) < turn(a)) | (j == 1) | (j == ny - 1)

        y_now = jnp.int32(0)
        for j in range(1, ny):
            v = ring(y + j, ny)
            y_now = y_now + awaits(y, v, j).astype(jnp.int32)

            @pl.when(awaits(v, y, j))
            def _(v=v):
                tell(barrier, "mp", v)

        each(nz, tell_z(barrier), rank_z + 1)
        each(nx, tell_x(barrier), rank_x + 1)

        @pl.when(c == 1)
        def _():
            tell(barrier, "dp_2", other)

        def next_slices(i):
            slice_in(i).start()
            slice_in(in_half + i).start()

        each(in_half, next_slices, 1)
        each(ny, lambda j: text_in(ring(y + near + j, ny), 6).start(), 1)
        load(gain_h, gain, 4).start()
        load(vis_h, vis, 2).start()
        each(ny, lambda k: img_in(k).start())
        load(text_h, txt, 3).start()
        load(count_h, count_s, 8).start()

        def owner_of(way, d):
            return ring(y + d, ny) if way == 0 else ring(y + ny - d, ny)

        def text_dot(owner, s):
            cols = qw[pl.ds(pl.multiple_of(s * tw, tw), tw), :]
            return dot_nt(qt[owner], cols)

        def text_send(way, d, h, k):
            s = h * in_half + k
            return send(
                tb.at[way, d * slices + s],
                tb.at[way, (d - 1) * slices + s],
                ts_s.at[way],
                arrival(way, d - 1, h, k),
                "mp",
                ring(y + 1, ny) if way == 0 else ring(y + ny - 1, ny),
            )

        def text_first(i):
            far = i < in_half
            k = lax.rem(i, in_half)
            for way in (0, 1):
                h = jnp.where(far, way, 1 - way)
                d = jnp.where(far, near, near - 1)
                s = h * in_half + k
                tb[way, d * slices + s] = text_dot(owner_of(way, d), s).astype(BF16)
                text_send(way, d, h, k).start()

        def text_next_first(i):
            @pl.when(i < in_half)
            def _():
                pair_wait(i)

            text_first(i)

        def text_relay(n):
            u = n // in_half
            k = lax.rem(n, in_half)
            d = near - 1 - (u + 1) // 2
            for way in (0, 1):
                h = lax.rem(u + way, 2)
                s = h * in_half + k
                slot = d * slices + s
                mine = text_dot(owner_of(way, d), s)

                @pl.when(lax.rem(k, 2) == 0)
                def _(way=way, d=d, h=h, k=k):
                    drain(tb.at[way, pl.ds(0, 2)], arrival(way, d, h, k))

                tb[way, slot] = (mine + tb[way, slot].astype(F32)).astype(BF16)
                text_send(way, d, h, k).start()

        steps = (ny - 3) * in_half
        firsts = 2 * in_half
        place = jnp.where(y < near, y, ny + near - 1 - y)
        begins = jnp.where(z < 7, 35 + 14 * z, 110 + 3 * z)
        begins += jnp.where(y < near, 6 * y - 30, 3 * (place - near) - 10)
        begins += jnp.where(x < 2, 5 * x - 10, 0) - 4 * c
        ahead = jnp.clip((SLACK - begins) // 21, 0, LEAD)
        out = [jnp.int32(1), 1]

        def pace(n, most=None, times=1, more=0):
            most = min(n + LEAD if most is None else most, pieces)
            upto = jnp.minimum(n + times * ahead + more, most)
            upto = jnp.maximum(upto, out[0])
            if out[1] < firsts:
                each(jnp.minimum(upto, firsts), text_next_first, jnp.minimum(out[0], firsts))
            if most > firsts:
                each(jnp.maximum(upto, firsts) - firsts, text_relay, jnp.maximum(out[0], firsts) - firsts)
            out[0], out[1] = upto, max(out[1], min(n, pieces))

        def text_near(k):
            @pl.when(k == 0)
            def _():
                for way in (0, 1):
                    drain(tb.at[way, pl.ds(0, in_half)], arrival(way, 0, 1 - way, 0))

            for h in (0, 1):
                s = h * in_half + k
                gtxt[s] = text_dot(y, s) + tb[1 - h, s].astype(F32)

        def agz(k):
            ref = ag.at[k, c, x, z]
            return lambda j: send(ref, ref, agz_s, agz_r.at[k], "dp_0", ring(z + j, nz))

        def agx(k):
            ref = ag.at[k, c, x, pl.ds(0, live_z)]
            return lambda j: send(ref, ref, agx_s, agx_r.at[k], "dp_1", ring(x + j, nx))

        def agc(k):
            ref = ag.at[k, c]
            return send(ref, ref, agc_s, agc_r.at[k], "dp_2", other)

        def agz_wait(k):
            drain(ag.at[0, 0, 0, pl.ds(0, nz - 1)], agz_r.at[k])

        def agx_wait(k):
            drain(ag.at[0, 0, pl.ds(0, nx - 1), pl.ds(0, live_z)], agx_r.at[k])

        def agc_wait(k):
            drain(ag.at[0, 0], agc_r.at[k])

        def rc(k):
            live = pl.ds(0, live_z)
            return send(
                hs.at[k, other, :, live], hc.at[k, :, live], rc_s, rc_r.at[k], "dp_2", other
            )

        side_z = min(2, (nz - 1) // 2)
        near_z = 2 * side_z + 1
        runs = (pl.ds(near_z, nz - near_z), pl.ds(0, near_z))
        FAR, NEAR = 0, 1

        def slot_z(zz):
            return ring(zz - z + side_z + nz, nz)

        def rx(k, part):
            def one(j):
                to = ring(x + j, nx)
                src, dst = h1.at[k, to, runs[part]], hx.at[k, j - 1, runs[part]]
                return send(src, dst, rx_s, rx_r.at[k, part], "dp_1", to)

            begin(one, nx)

        def rz(k, part):
            def one(off):
                to = ring(z + off + nz, nz)
                return send(
                    h2.at[k, off + side_z], hz.at[k, off + side_z], rz_s, rz_r.at[k], "dp_0", to
                )

            if part == NEAR:
                for off in range(side_z, 0, -1):
                    one(off).start()
                    one(-off).start()
                return

            def by_side(i):
                one(nz // 2 + jnp.where(lax.rem(i, 2) == 1, (i + 1) // 2, -(i // 2))).start()

            each(nz - near_z, by_side)

        def st_send(k):
            return lambda j: send(
                st.at[k], st_in.at[k, j - 1], st_s, st_r.at[k], "mp", ring(y + j, ny)
            )

        def sy_send(j):
            return send(sy.at[y], sy.at[y], sy_s, sy_r, "mp", ring(y + j, ny))

        def ty_send(j):
            to = ring(y + j, ny)
            return send(ty.at[to], ty_in.at[j - 1], ty_s, ty_r, "mp", to)

        def place(zz, r):
            return pl.ds(pl.multiple_of((zz * 2 * nx + r) * shard, 16), shard)

        def unpack(k):
            def one(zz):
                for r in range(2 * nx):
                    flat[place(zz, r), :] = ag[k, r % 2, r // 2, zz].astype(F32)

            each(live_z, one)
            for q in range(packed):
                wblk[:, q * LANES : (q + 1) * LANES] = flat[pl.ds(q, enc, packed), :].astype(BF16)

        def pack(k, block):
            for q in range(packed):
                flat[pl.ds(q, enc, packed), :] = block[:, q * LANES : (q + 1) * LANES]
            end = live_z * 2 * nx * shard
            if end > enc * packed:
                flat[enc * packed : end, :] = jnp.zeros((end - enc * packed, LANES), F32)

            def one(zz):
                for r in range(2 * nx):
                    hs[k, r % 2, r // 2, zz] = flat[place(zz, r), :].astype(BF16)

            each(live_z, one)

        def core_sum(k):
            rc(k).wait_recv()

            def one(zz):
                for xx in range(nx):
                    pair = hs[k, c, xx, zz].astype(F32) + hc[k, xx, zz].astype(F32)
                    h1[k, xx, slot_z(zz)] = pair.astype(BF16)

            each(live_z, one)

        def x_sum(k, part):
            drain(hx.at[k, :, runs[part]], rx_r.at[k, part])

            def one(slot):
                acc = h1[k, x, slot].astype(F32)
                for j in range(nx - 1):
                    acc = acc + hx[k, j, slot].astype(F32)
                h2[k, slot] = acc.astype(BF16)

            lo, hi = (near_z, nz) if part == FAR else (0, near_z)
            each(hi, one, lo)
            rz(k, part)

        def z_sum(k):
            drain(hz.at[k, pl.ds(0, nz - 1)], rz_r.at[k])
            acc = h2[k, side_z].astype(F32)
            for slot in range(nz):
                if slot != side_z:
                    acc = acc + hz[k, slot].astype(F32)
            return acc

        def publish(k, column):
            wide = jnp.broadcast_to(column, (img_all, LANES))
            st[k] = wide.T[0:1, :]
            begin(st_send(k), ny)

        def collected(k):
            drain(st_in.at[k], st_r.at[k])
            row = st[k]
            for j in range(ny - 1):
                row = row + st_in[k, j]
            return jnp.broadcast_to(row, (LANES, img_all)).T[:, 0:1]

        def text_ahead(way):
            tb[way, near * slices + way * in_half] = text_dot(owner_of(way, near), way * in_half).astype(BF16)

        pair_wait(0)
        text_in(ring(y + near, ny), 5).wait()
        text_ahead(0)
        pl.semaphore_wait(barrier, y_now + rank_z + rank_x + other)
        each(rank_z, tell_z(in_sem))
        text_send(0, near, 0, 0).start()
        text_ahead(1)
        text_send(1, near, 1, 0).start()
        each(rank_x, tell_x(in_sem))
        load(proj_h, sy.at[y], 1).wait()

        @pl.when(c == 0)
        def _():
            tell(in_sem, "dp_2", other)

        for j in range(1, ny):
            v = ring(y + j, ny)

            @pl.when(jnp.logical_not(awaits(v, y, j)))
            def _(v=v):
                tell(y_sem, "mp", v)

        load(proj_h, ag.at[0, c, x, z], 0).wait()
        drain(qt.at[pl.ds(0, ny - 1)], load_sem.at[6])

        early = z < EARLY
        pace(1, 3, 0, (ny - 1 - turn(y)) // 3)

        @pl.when(y_now < ny - 1)
        def _():
            pl.semaphore_wait(y_sem, ny - 1 - y_now)

        begin(sy_send, ny)
        pace(1, firsts + 2, 2)
        rest = (nz - 1 - rank_z) + (nx - 1 - rank_x) + c

        @pl.when(rest > 0)
        def _():
            pl.semaphore_wait(in_sem, rest)

        begin(agz(0), nz)
        rows_f[...] = jnp.zeros(rows_f.shape, F32)
        cross_f[...] = jnp.zeros(cross_f.shape, F32)
        for k in (0, 1):
            for zz in range(live_z, nz):
                h1[k, :, slot_z(zz)] = jnp.zeros((nx, shard, LANES), BF16)
        pace(4)
        load(vis_h, vis, 2).wait()
        vis_t[...] = vis[...].T
        pace(6)
        agz_wait(0)
        begin(agx(0), nx)

        load(gain_h, gain, 4).wait()
        drain(sy.at[pl.ds(0, ny - 1)], sy_r)
        for m in range(ny):
            rows_f[m, 0:shard, :] = sy[m].astype(F32)
            for q in range(packed):
                cols = slice(m * width + q * LANES, m * width + (q + 1) * LANES)
                piece = rows_f[m, pl.ds(q, own_rows, packed), :] * gain[:, cols]
                lhs[:, cols] = piece.astype(BF16)
        prod = jnp.dot(lhs[...], qw[...], preferred_element_type=F32)
        for q in range(packed):
            rows_f[0, pl.ds(q, own_rows, packed), :] = prod[:, q * LANES : (q + 1) * LANES]
        ag[1, c, x, z] = rows_f[0, 0:shard, :].astype(BF16)
        begin(agz(1), nz)
        pace(9)
        agx_wait(0)
        agc(0).start()

        drain(qi, load_sem.at[7])
        agz_wait(1)
        begin(agx(1), nx)
        agc_wait(0)
        unpack(0)
        embed = jnp.dot(vis[...], wblk[...], preferred_element_type=F32).astype(BF16)
        emb[...] = embed
        embed = embed.astype(F32)
        publish(0, jnp.sum(embed * embed, axis=1, keepdims=True))
        pace(13)

        agx_wait(1)
        agc(1).start()
        agc_wait(1)
        unpack(1)
        back = jnp.dot(vis[...], wblk[...], preferred_element_type=F32)
        publish(1, jnp.sum(back * qi[...].astype(F32), axis=1, keepdims=True))
        pace(14)

        load(count_h, count_s, 8).wait()
        row = lax.broadcasted_iota(jnp.int32, (img_all, 1), 0)
        counts = jnp.zeros((img_all, 1), jnp.int32)
        for k in range(ny):
            counts = jnp.where(row // IMG == k, count_s[k], counts)
        live = lax.rem(row, IMG) // PATCH < counts
        inv = lax.rsqrt(collected(0) * per_row + EPS)
        left = jnp.where(live, inv * qi[...].astype(F32), 0.0).astype(BF16)
        pack(0, jnp.dot(vis_t[...], left, preferred_element_type=F32))
        rc(0).start()
        pace(16)
        core_sum(0)
        rx(0, FAR)
        rx(0, NEAR)
        pace(17)

        mean = collected(1) * per_row
        right = jnp.where(live, (inv * inv * inv * mean) * emb[...].astype(F32), 0.0).astype(BF16)
        pack(1, jnp.dot(vis_t[...], right, preferred_element_type=F32))
        rc(1).start()
        pace(19)
        core_sum(1)
        rx(1, FAR)
        rx(1, NEAR)
        x_sum(0, FAR)
        pace(20)

        load(text_h, txt, 3).wait()
        sq_t = jnp.zeros((text_rows, 1), F32)
        for s in range(slices):
            rows_t = txt[:, s * tw : (s + 1) * tw].astype(F32)
            sq_t = sq_t + jnp.sum(rows_t * rows_t, axis=1, keepdims=True)
        sq_f[...] = jnp.broadcast_to(sq_t, sq_f.shape)
        x_sum(0, NEAR)
        pace(22)
        x_sum(1, FAR)
        pace(24, pieces - 2)

        rows_f[0, 0:shard, :] = z_sum(0)
        for q in range(packed):
            lhs[:, q * LANES : (q + 1) * LANES] = rows_f[0, pl.ds(q, own_rows, packed), :].astype(BF16)
        term = lhs[:, 0:width]
        for m in range(ny):
            prod = dot_nt(term, qw[m * width : (m + 1) * width, :])
            for q in range(packed):
                rows_f[m, pl.ds(q, own_rows, packed), :] = prod[:, q * LANES : (q + 1) * LANES]
            ty[m] = rows_f[m, 0:shard, :].astype(BF16)
        begin(ty_send, ny)
        x_sum(1, NEAR)
        pace(pieces)
        each(in_half, text_near)
        first_part = jnp.where(early, in_half, 0)
        each(first_part, text_last)
        second = z_sum(1)
        drain(ty_in, ty_r)
        one_term = ty[y].astype(F32)
        for j in range(ny - 1):
            one_term = one_term + ty_in[j].astype(F32)
        at = lax.rem(lax.broadcasted_iota(jnp.int32, (shard, LANES), 0), packed)
        gain_own = jnp.zeros((shard, LANES), F32)
        for q in range(packed):
            cols = pl.ds(pl.multiple_of(y * width + q * LANES, LANES), LANES)
            gain_own = jnp.where(at == q, gain[:, cols], gain_own)
        proj_o[...] = (gain_own * one_term - second) * (float(nz * nx * 2 * img_all) ** -0.5)
        drain(sy.at[pl.ds(0, ny - 1)], sy_s)
        drain(ag.at[0, 0, pl.ds(0, 2), pl.ds(0, nz - 1)], agz_s)
        drain(ag.at[:, 0, pl.ds(0, nx - 1), pl.ds(0, live_z)], agx_s)
        drain(ag.at[0], agc_s)
        drain(st_in, st_s)
        drain(hc.at[:, :, pl.ds(0, live_z)], rc_s)
        drain(hx, rx_s)
        drain(hz.at[:, pl.ds(0, nz - 1)], rz_s)
        drain(ty_in, ty_s)

    sem = pltpu.SemaphoreType.DMA
    pl.run_scoped(
        work,
        pltpu.SemaphoreType.REGULAR,
        pltpu.SemaphoreType.REGULAR,
        sem((9 + in_half,)),
        sem,
        sem,
        *([sem, sem((2,))] * 3),
        *([sem, sem((2,))] * 2),
        sem,
        sem((2, 2)),
        sem,
        sem((2,)),
        sem,
        sem,
    )

    each(in_half, text_last, jnp.where(lax.axis_index("dp_0") < EARLY, in_half, 0))

    cross_t = jnp.sum(cross_f[...], axis=1, keepdims=True)
    inv_t = lax.rsqrt(sq_f[:, 0:1] * per_row + EPS)
    scale_t = inv_t * inv_t * inv_t * (cross_t * per_row)
    for s in range(slices):
        cols = slice(s * tw, (s + 1) * tw)
        text_o[:, cols] = (inv_t * gtxt[s] - txt[:, cols].astype(F32) * scale_t).astype(BF16)

    for way in (0, 1):
        drain(tb.at[way, pl.ds(0, pieces)], ts_s.at[way])


def put_out(text_v, proj_v, text_o, proj_o, sems):
    a = pltpu.make_async_copy(text_v, text_o, sems.at[0])
    b = pltpu.make_async_copy(proj_v, proj_o, sems.at[1])
    a.start()
    b.start()
    a.wait()
    b.wait()


def body(vision_rows, image_count, proj_flat, text_embeds, norm_gain, q_weight, q_grad):
    nz, nx, ny = (lax.axis_size(a) for a in ("dp_0", "dp_1", "mp"))
    total, width = q_weight.shape
    img_all, enc = vision_rows.shape
    text_rows = text_embeds.shape[0]
    shard = proj_flat.shape[0]
    packed = width // LANES
    own_rows = -(-shard // packed // 16) * 16
    near = ny // 2
    slices = 8
    tw = total // slices
    flat_rows = nz * nx * 2 * shard
    sem = pltpu.SemaphoreType.DMA
    any_space = pl.BlockSpec(memory_space=pl.ANY)
    in_vmem = pl.BlockSpec(memory_space=pltpu.VMEM)
    scratch = [
        pltpu.VMEM((total, width), BF16),
        pltpu.VMEM((img_all, width), BF16),
        pltpu.VMEM((ny, text_rows, width), BF16),
        pltpu.VMEM((img_all, enc), BF16),
        pltpu.VMEM((enc, img_all), BF16),
        pltpu.VMEM((text_rows, total), BF16),
        pltpu.VMEM((1, total), F32),
        pltpu.VMEM((ny, shard, LANES), BF16),
        pltpu.VMEM((ny, own_rows * packed, LANES), F32),
        pltpu.VMEM((own_rows, total), BF16),
        pltpu.VMEM((2, 2, nx, nz, shard, LANES), BF16),
        pltpu.VMEM((flat_rows, LANES), F32),
        pltpu.VMEM((enc, width), BF16),
        pltpu.VMEM((img_all, width), BF16),
        pltpu.VMEM((2, (near + 1) * slices, text_rows, tw), BF16),
        pltpu.VMEM((slices, text_rows, tw), F32),
        pltpu.VMEM((text_rows, LANES), F32),
        pltpu.VMEM((text_rows, LANES), F32),
        pltpu.VMEM((2, 1, img_all), F32),
        pltpu.VMEM((2, ny - 1, 1, img_all), F32),
        pltpu.VMEM((2, 2, nx, nz, shard, LANES), BF16),
        pltpu.VMEM((2, nx, nz, shard, LANES), BF16),
        pltpu.VMEM((2, nx, nz, shard, LANES), BF16),
        pltpu.VMEM((2, nx - 1, nz, shard, LANES), BF16),
        pltpu.VMEM((2, nz, shard, LANES), BF16),
        pltpu.VMEM((2, nz, shard, LANES), BF16),
        pltpu.VMEM((ny, shard, LANES), BF16),
        pltpu.VMEM((ny - 1, shard, LANES), BF16),
        pltpu.SMEM((ny,), jnp.int32),
        sem((2,)),
        sem((2, (near - 1) * slices // 2 + 1 + slices // 2)),
    ]
    text_v, proj_v = pl.pallas_call(
        functools.partial(kernel, (nz, nx, ny)),
        out_shape=(pltpu.VMEM(text_embeds.shape, BF16), pltpu.VMEM(proj_flat.shape, F32)),
        in_specs=[any_space] * 7,
        out_specs=(in_vmem, in_vmem),
        scratch_shapes=scratch,
        compiler_params=pltpu.CompilerParams(
            collective_id=0,
            has_side_effects=True,
            vmem_limit_bytes=56 * 1024 * 1024,
        ),
        name="step",
    )(vision_rows, image_count, proj_flat, text_embeds, norm_gain.reshape(1, -1), q_weight, q_grad)
    return pl.pallas_call(
        put_out,
        out_shape=(
            jax.ShapeDtypeStruct(text_embeds.shape, BF16),
            jax.ShapeDtypeStruct(proj_flat.shape, F32),
        ),
        in_specs=[in_vmem] * 2,
        out_specs=(any_space, any_space),
        scratch_shapes=[sem((2,))],
        name="put_out",
    )(*(pltpu.with_memory_space_constraint(v, pltpu.VMEM) for v in (text_v, proj_v)))


def solution(mesh):
    finer = Mesh(mesh.devices.reshape(12, 4, 2, mesh.shape["mp"]), ("dp_0", "dp_1", "dp_2", "mp"))
    placed = (P(DP, None), P(DP), P(DP_MP, None), P(DP_MP, None), P(), P(None, "mp"), P(DP, "mp"))
    return jax.shard_map(
        body,
        mesh=finer,
        in_specs=placed,
        out_specs=(P(DP_MP, None), P(DP_MP, None)),
        check_vma=False,
    )
```

```python
import functools

import jax
import jax.numpy as jnp
from jax import lax
from jax.experimental import pallas as pl
from jax.experimental.pallas import tpu as pltpu
from jax.sharding import Mesh
from jax.sharding import PartitionSpec as P

IMG_MAX = 4
PATCH = 8
IMG = IMG_MAX * PATCH
LANES = 128
DP = ("dp_0", "dp_1", "dp_2")
DP_MP = ("dp_0", "dp_1", "dp_2", "mp")
EPS = 1e-05
LEAD = 7
SLACK = 148
EARLY = 3
MESH = pl.DeviceIdType.MESH
F32 = jnp.float32
BF16 = jnp.bfloat16


def dot_nt(a, b):
    return lax.dot_general(a, b, (((1,), (1,)), ((), ())), preferred_element_type=F32)


def kernel(
    sizes,
    vis_h,
    count_h,
    proj_h,
    text_h,
    gain_h,
    qw_h,
    qg_h,
    text_o,
    proj_o,
    qw,
    qw_t,
    qi,
    qt,
    vis,
    vis_t,
    txt,
    gain,
    sy,
    rows_f,
    lhs,
    ag,
    flat,
    wblk,
    emb,
    tb,
    gtxt,
    cross_f,
    sq_f,
    st,
    st_in,
    hs,
    hc,
    h1,
    hx,
    h2,
    hz,
    ty,
    ty_in,
    count_s,
    ts_s,
    ts_r,
):
    nz, nx, ny = sizes
    text_rows, total = txt.shape
    near = ny // 2
    slices = gtxt.shape[0]
    in_half = slices // 2
    tw = tb.shape[3]
    per_row = 1.0 / total
    pieces = 2 * in_half + (ny - 3) * in_half
    mid_sems = (near - 1) * slices // 2

    def drain(ref, sem):
        pltpu.make_async_copy(ref, ref, sem).wait()

    def each(n, act, lo=0):
        def one(k, carry):
            act(k)
            return carry

        lax.fori_loop(lo, n, one, 0)

    def arrival(way, d, h, k):
        mid = ((d - 1) * slices + h * in_half + k) // 2
        end = mid_sems + jnp.where(h == way, 1 + k, 0)
        return ts_r.at[way, jnp.where(d > 0, mid, end)]

    def text_last(k):
        for h in (0, 1):
            s = h * in_half + k
            drain(tb.at[h, 0], arrival(h, 0, h, k))
            cols = pl.ds(pl.multiple_of(s * tw, LANES), tw)
            g = (gtxt[s] + tb[h, s].astype(F32)) * gain[:, cols]
            gtxt[s] = g
            prod = g * txt[:, cols].astype(F32)
            for q in range(tw // LANES):
                cross_f[...] += prod[:, q * LANES : (q + 1) * LANES]

    def work(
        in_sem,
        y_sem,
        load_sem,
        sy_s,
        sy_r,
        agz_s,
        agz_r,
        agx_s,
        agx_r,
        agc_s,
        agc_r,
        st_s,
        st_r,
        rc_s,
        rc_r,
        rx_s,
        rx_r,
        rz_s,
        rz_r,
        ty_s,
        ty_r,
    ):
        z = lax.axis_index("dp_0")
        x = lax.axis_index("dp_1")
        c = lax.axis_index("dp_2")
        y = lax.axis_index("mp")
        width = qw.shape[1]
        enc = vis.shape[1]
        img_all = qi.shape[0]
        packed = width // LANES
        shard = proj_h.shape[0]
        own_rows = lhs.shape[0]
        live_z = -(-enc * packed // (2 * nx * shard))
        other = 1 - c

        def ring(i, n):
            return lax.rem(i, n)

        def begin(make, n):
            def one(i, carry):
                side = jnp.where(lax.rem(i, 2) == 1, (i + 1) // 2, -(i // 2))
                make(n // 2 + side).start()
                return carry

            lax.fori_loop(0, n - 1, one, 0)

        def send(src, dst, send_sem, recv_sem, axis, index):
            return pltpu.make_async_remote_copy(
                src_ref=src,
                dst_ref=dst,
                send_sem=send_sem,
                recv_sem=recv_sem,
                device_id={axis: index},
                device_id_type=MESH,
            )

        def load(src, dst, i):
            return pltpu.make_async_copy(src, dst, load_sem.at[i])

        rows_each = IMG + text_rows

        def text_in(k, i):
            base = pl.multiple_of(k * rows_each + IMG, 16)
            return load(qg_h.at[pl.ds(base, text_rows)], qt.at[k], i)

        def img_in(k):
            base = pl.multiple_of(k * rows_each, 16)
            to = qi.at[pl.ds(pl.multiple_of(k * IMG, 16), IMG)]
            return load(qg_h.at[pl.ds(base, IMG)], to, 7)

        def slice_in(s):
            cols = pl.ds(pl.multiple_of(s * tw, tw), tw)
            return load(qw_h.at[cols], qw.at[cols], 9 + lax.rem(s, in_half))

        def pair_wait(i):
            drain(qw.at[pl.ds(0, 2 * tw)], load_sem.at[9 + i])

        slice_in(0).start()
        text_in(ring(y + near, ny), 5).start()
        slice_in(in_half).start()
        load(proj_h, ag.at[0, c, x, z], 0).start()
        load(proj_h, sy.at[y], 1).start()

        barrier = pltpu.get_barrier_semaphore()

        def tell(what, axis, index):
            pl.semaphore_signal(what, inc=1, device_id={axis: index}, device_id_type=MESH)

        corner_z = ((x == 0) & (y == 0) & (c == 0)).astype(jnp.int32)
        corner_x = ((z == 0) & (y == 0) & (c == 0)).astype(jnp.int32)
        corner_y = ((z == 0) & (x == 0) & (c == 0)).astype(jnp.int32)
        rank_z = ring(z + nz - corner_z, nz)
        rank_x = ring(x + nx - corner_x, nx)

        def tell_z(what):
            return lambda r: tell(what, "dp_0", ring(r + corner_z, nz))

        def tell_x(what):
            return lambda r: tell(what, "dp_1", ring(r + corner_x, nx))

        def turn(v):
            place = jnp.where(v < near, v, ny + near - 1 - v)
            place = jnp.where(place == near, near - 1, jnp.where(place == near - 1, near, place))
            return ring(place + ny - corner_y, ny)

        def awaits(a, b, j):
            return (turn(b) < turn(a)) | (j == 1) | (j == ny - 1)

        y_now = jnp.int32(0)
        for j in range(1, ny):
            v = ring(y + j, ny)
            y_now = y_now + awaits(y, v, j).astype(jnp.int32)

            @pl.when(awaits(v, y, j))
            def _(v=v):
                tell(barrier, "mp", v)

        each(nz, tell_z(barrier), rank_z + 1)
        each(nx, tell_x(barrier), rank_x + 1)

        @pl.when(c == 1)
        def _():
            tell(barrier, "dp_2", other)

        def next_slices(i):
            slice_in(i).start()
            slice_in(in_half + i).start()

        each(in_half, next_slices, 1)
        each(ny, lambda j: text_in(ring(y + near + j, ny), 6).start(), 1)
        load(gain_h, gain, 4).start()
        load(vis_h, vis, 2).start()
        each(ny, lambda k: img_in(k).start())
        load(text_h, txt, 3).start()
        load(count_h, count_s, 8).start()

        def owner_of(way, d):
            return ring(y + d, ny) if way == 0 else ring(y + ny - d, ny)

        def text_dot(owner, s, turned=False):
            cols = pl.ds(pl.multiple_of(s * tw, tw), tw)
            if turned:
                return jnp.dot(qt[owner], qw_t[:, cols], preferred_element_type=F32)
            return dot_nt(qt[owner], qw[cols, :])

        def turn_weight():
            def one(s):
                cols = pl.ds(pl.multiple_of(s * tw, tw), tw)
                qw_t[:, cols] = qw[cols, :].T

            each(slices, one)

        def text_send(way, d, h, k):
            s = h * in_half + k
            return send(
                tb.at[way, d * slices + s],
                tb.at[way, (d - 1) * slices + s],
                ts_s.at[way],
                arrival(way, d - 1, h, k),
                "mp",
                ring(y + 1, ny) if way == 0 else ring(y + ny - 1, ny),
            )

        def text_first(i):
            far = i < in_half
            k = lax.rem(i, in_half)
            for way in (0, 1):
                h = jnp.where(far, way, 1 - way)
                d = jnp.where(far, near, near - 1)
                s = h * in_half + k
                tb[way, d * slices + s] = text_dot(owner_of(way, d), s).astype(BF16)
                text_send(way, d, h, k).start()

        def text_next_first(i):
            @pl.when(i < in_half)
            def _():
                pair_wait(i)

            text_first(i)

        def text_relay(n, turned):
            u = n // in_half
            k = lax.rem(n, in_half)
            d = near - 1 - (u + 1) // 2
            for way in (0, 1):
                h = lax.rem(u + way, 2)
                s = h * in_half + k
                slot = d * slices + s
                mine = text_dot(owner_of(way, d), s, turned)

                @pl.when(lax.rem(k, 2) == 0)
                def _(way=way, d=d, h=h, k=k):
                    drain(tb.at[way, pl.ds(0, 2)], arrival(way, d, h, k))

                tb[way, slot] = (mine + tb[way, slot].astype(F32)).astype(BF16)
                text_send(way, d, h, k).start()

        steps = (ny - 3) * in_half
        firsts = 2 * in_half
        place = jnp.where(y < near, y, ny + near - 1 - y)
        begins = jnp.where(z < 7, 35 + 14 * z, 110 + 3 * z)
        begins += jnp.where(y < near, 6 * y - 30, 3 * (place - near) - 10)
        begins += jnp.where(x < 2, 5 * x - 10, 0) + c
        ahead = jnp.clip((SLACK - begins) // 21, 0, LEAD)
        out = [jnp.int32(1), 1]

        def pace(n, most=None, times=1, more=0, turned=True):
            most = min(n + LEAD if most is None else most, pieces)
            upto = jnp.minimum(n + times * ahead + more, most)
            upto = jnp.maximum(upto, out[0])
            if out[1] < firsts:
                each(jnp.minimum(upto, firsts), text_next_first, jnp.minimum(out[0], firsts))
            if most > firsts:
                each(jnp.maximum(upto, firsts) - firsts, lambda n: text_relay(n, turned), jnp.maximum(out[0], firsts) - firsts)
            out[0], out[1] = upto, max(out[1], min(n, pieces))

        def text_near(k):
            @pl.when(k == 0)
            def _():
                for way in (0, 1):
                    drain(tb.at[way, pl.ds(0, in_half)], arrival(way, 0, 1 - way, 0))

            for h in (0, 1):
                s = h * in_half + k
                gtxt[s] = text_dot(y, s, True) + tb[1 - h, s].astype(F32)

        def agz(k):
            ref = ag.at[k, c, x, z]
            return lambda j: send(ref, ref, agz_s, agz_r.at[k], "dp_0", ring(z + j, nz))

        def agx(k):
            ref = ag.at[k, c, x, pl.ds(0, live_z)]
            return lambda j: send(ref, ref, agx_s, agx_r.at[k], "dp_1", ring(x + j, nx))

        def agc(k):
            ref = ag.at[k, c]
            return send(ref, ref, agc_s, agc_r.at[k], "dp_2", other)

        def agz_wait(k):
            drain(ag.at[0, 0, 0, pl.ds(0, nz - 1)], agz_r.at[k])

        def agx_wait(k):
            drain(ag.at[0, 0, pl.ds(0, nx - 1), pl.ds(0, live_z)], agx_r.at[k])

        def agc_wait(k):
            drain(ag.at[0, 0], agc_r.at[k])

        def rc(k):
            live = pl.ds(0, live_z)
            return send(
                hs.at[k, other, :, live], hc.at[k, :, live], rc_s, rc_r.at[k], "dp_2", other
            )

        side_z = min(2, (nz - 1) // 2)
        near_z = 2 * side_z + 1
        runs = (pl.ds(near_z, nz - near_z), pl.ds(0, near_z))
        FAR, NEAR = 0, 1

        def slot_z(zz):
            return ring(zz - z + side_z + nz, nz)

        def rx(k, part):
            def one(j):
                to = ring(x + j, nx)
                src, dst = h1.at[k, to, runs[part]], hx.at[k, j - 1, runs[part]]
                return send(src, dst, rx_s, rx_r.at[k, part], "dp_1", to)

            begin(one, nx)

        def rz(k, part):
            def one(off):
                to = ring(z + off + nz, nz)
                return send(
                    h2.at[k, off + side_z], hz.at[k, off + side_z], rz_s, rz_r.at[k], "dp_0", to
                )

            if part == NEAR:
                for off in range(side_z, 0, -1):
                    one(off).start()
                    one(-off).start()
                return

            def by_side(i):
                one(nz // 2 + jnp.where(lax.rem(i, 2) == 1, (i + 1) // 2, -(i // 2))).start()

            each(nz - near_z, by_side)

        def st_send(k):
            return lambda j: send(
                st.at[k], st_in.at[k, j - 1], st_s, st_r.at[k], "mp", ring(y + j, ny)
            )

        def sy_send(j):
            return send(sy.at[y], sy.at[y], sy_s, sy_r, "mp", ring(y + j, ny))

        def ty_send(j):
            to = ring(y + j, ny)
            return send(ty.at[to], ty_in.at[j - 1], ty_s, ty_r, "mp", to)

        def place(zz, r):
            return pl.ds(pl.multiple_of((zz * 2 * nx + r) * shard, 16), shard)

        def unpack(k):
            def one(zz):
                for r in range(2 * nx):
                    flat[place(zz, r), :] = ag[k, r % 2, r // 2, zz].astype(F32)

            each(live_z, one)
            for q in range(packed):
                wblk[:, q * LANES : (q + 1) * LANES] = flat[pl.ds(q, enc, packed), :].astype(BF16)

        def pack(k, block):
            for q in range(packed):
                flat[pl.ds(q, enc, packed), :] = block[:, q * LANES : (q + 1) * LANES]
            end = live_z * 2 * nx * shard
            if end > enc * packed:
                flat[enc * packed : end, :] = jnp.zeros((end - enc * packed, LANES), F32)

            def one(zz):
                for r in range(2 * nx):
                    hs[k, r % 2, r // 2, zz] = flat[place(zz, r), :].astype(BF16)

            each(live_z, one)

        def core_sum(k):
            rc(k).wait_recv()

            def one(zz):
                for xx in range(nx):
                    pair = hs[k, c, xx, zz].astype(F32) + hc[k, xx, zz].astype(F32)
                    h1[k, xx, slot_z(zz)] = pair.astype(BF16)

            each(live_z, one)

        def x_sum(k, part):
            drain(hx.at[k, :, runs[part]], rx_r.at[k, part])

            def one(slot):
                acc = h1[k, x, slot].astype(F32)
                for j in range(nx - 1):
                    acc = acc + hx[k, j, slot].astype(F32)
                h2[k, slot] = acc.astype(BF16)

            lo, hi = (near_z, nz) if part == FAR else (0, near_z)
            each(hi, one, lo)
            rz(k, part)

        def z_sum(k):
            drain(hz.at[k, pl.ds(0, nz - 1)], rz_r.at[k])
            acc = h2[k, side_z].astype(F32)
            for slot in range(nz):
                if slot != side_z:
                    acc = acc + hz[k, slot].astype(F32)
            return acc

        def publish(k, column):
            wide = jnp.broadcast_to(column, (img_all, LANES))
            st[k] = wide.T[0:1, :]
            begin(st_send(k), ny)

        def collected(k):
            drain(st_in.at[k], st_r.at[k])
            row = st[k]
            for j in range(ny - 1):
                row = row + st_in[k, j]
            return jnp.broadcast_to(row, (LANES, img_all)).T[:, 0:1]

        def text_ahead(way):
            tb[way, near * slices + way * in_half] = text_dot(owner_of(way, near), way * in_half).astype(BF16)

        pair_wait(0)
        text_in(ring(y + near, ny), 5).wait()
        text_ahead(0)
        pl.semaphore_wait(barrier, y_now + rank_z + rank_x + other)
        each(rank_z, tell_z(in_sem))
        text_send(0, near, 0, 0).start()
        text_ahead(1)
        text_send(1, near, 1, 0).start()
        each(rank_x, tell_x(in_sem))
        load(proj_h, sy.at[y], 1).wait()

        @pl.when(c == 0)
        def _():
            tell(in_sem, "dp_2", other)

        for j in range(1, ny):
            v = ring(y + j, ny)

            @pl.when(jnp.logical_not(awaits(v, y, j)))
            def _(v=v):
                tell(y_sem, "mp", v)

        load(proj_h, ag.at[0, c, x, z], 0).wait()
        drain(qt.at[pl.ds(0, ny - 1)], load_sem.at[6])

        early = z < EARLY
        pace(1, 3, 0, (ny - 1 - turn(y)) // 3, False)

        @pl.when(y_now < ny - 1)
        def _():
            pl.semaphore_wait(y_sem, ny - 1 - y_now)

        begin(sy_send, ny)
        pace(1, firsts + 2, 2, turned=False)
        rest = (nz - 1 - rank_z) + (nx - 1 - rank_x) + c

        @pl.when(rest > 0)
        def _():
            pl.semaphore_wait(in_sem, rest)

        begin(agz(0), nz)
        rows_f[...] = jnp.zeros(rows_f.shape, F32)
        cross_f[...] = jnp.zeros(cross_f.shape, F32)
        for k in (0, 1):
            for zz in range(live_z, nz):
                h1[k, :, slot_z(zz)] = jnp.zeros((nx, shard, LANES), BF16)
        pace(4, turned=False)
        load(vis_h, vis, 2).wait()
        vis_t[...] = vis[...].T
        pace(6, turned=False)
        turn_weight()
        agz_wait(0)
        begin(agx(0), nx)

        load(gain_h, gain, 4).wait()
        drain(sy.at[pl.ds(0, ny - 1)], sy_r)
        for m in range(ny):
            rows_f[m, 0:shard, :] = sy[m].astype(F32)
            for q in range(packed):
                cols = slice(m * width + q * LANES, m * width + (q + 1) * LANES)
                piece = rows_f[m, pl.ds(q, own_rows, packed), :] * gain[:, cols]
                lhs[:, cols] = piece.astype(BF16)
        prod = jnp.dot(lhs[...], qw[...], preferred_element_type=F32)
        for q in range(packed):
            rows_f[0, pl.ds(q, own_rows, packed), :] = prod[:, q * LANES : (q + 1) * LANES]
        ag[1, c, x, z] = rows_f[0, 0:shard, :].astype(BF16)
        begin(agz(1), nz)
        pace(9)
        agx_wait(0)
        agc(0).start()

        drain(qi, load_sem.at[7])
        agz_wait(1)
        begin(agx(1), nx)
        agc_wait(0)
        unpack(0)
        embed = jnp.dot(vis[...], wblk[...], preferred_element_type=F32).astype(BF16)
        emb[...] = embed
        embed = embed.astype(F32)
        publish(0, jnp.sum(embed * embed, axis=1, keepdims=True))
        pace(13)

        agx_wait(1)
        agc(1).start()
        agc_wait(1)
        unpack(1)
        back = jnp.dot(vis[...], wblk[...], preferred_element_type=F32)
        publish(1, jnp.sum(back * qi[...].astype(F32), axis=1, keepdims=True))
        pace(14)

        load(count_h, count_s, 8).wait()
        row = lax.broadcasted_iota(jnp.int32, (img_all, 1), 0)
        counts = jnp.zeros((img_all, 1), jnp.int32)
        for k in range(ny):
            counts = jnp.where(row // IMG == k, count_s[k], counts)
        live = lax.rem(row, IMG) // PATCH < counts
        inv = lax.rsqrt(collected(0) * per_row + EPS)
        left = jnp.where(live, inv * qi[...].astype(F32), 0.0).astype(BF16)
        pack(0, jnp.dot(vis_t[...], left, preferred_element_type=F32))
        rc(0).start()
        pace(16)
        core_sum(0)
        rx(0, FAR)
        rx(0, NEAR)
        pace(17)

        mean = collected(1) * per_row
        right = jnp.where(live, (inv * inv * inv * mean) * emb[...].astype(F32), 0.0).astype(BF16)
        pack(1, jnp.dot(vis_t[...], right, preferred_element_type=F32))
        rc(1).start()
        pace(19)
        core_sum(1)
        rx(1, FAR)
        rx(1, NEAR)
        x_sum(0, FAR)
        pace(20)

        load(text_h, txt, 3).wait()
        sq_t = jnp.zeros((text_rows, 1), F32)
        for s in range(slices):
            rows_t = txt[:, s * tw : (s + 1) * tw].astype(F32)
            sq_t = sq_t + jnp.sum(rows_t * rows_t, axis=1, keepdims=True)
        sq_f[...] = jnp.broadcast_to(sq_t, sq_f.shape)
        x_sum(0, NEAR)
        pace(22)
        x_sum(1, FAR)
        pace(24, pieces - 2)

        rows_f[0, 0:shard, :] = z_sum(0)
        for q in range(packed):
            lhs[:, q * LANES : (q + 1) * LANES] = rows_f[0, pl.ds(q, own_rows, packed), :].astype(BF16)
        term = lhs[:, 0:width]
        for m in range(ny):
            prod = jnp.dot(term, qw_t[:, m * width : (m + 1) * width], preferred_element_type=F32)
            for q in range(packed):
                rows_f[m, pl.ds(q, own_rows, packed), :] = prod[:, q * LANES : (q + 1) * LANES]
            ty[m] = rows_f[m, 0:shard, :].astype(BF16)
        begin(ty_send, ny)
        x_sum(1, NEAR)
        pace(pieces)
        each(in_half, text_near)
        first_part = jnp.where(early, in_half, 0)
        each(first_part, text_last)
        second = z_sum(1)
        drain(ty_in, ty_r)
        one_term = ty[y].astype(F32)
        for j in range(ny - 1):
            one_term = one_term + ty_in[j].astype(F32)
        at = lax.rem(lax.broadcasted_iota(jnp.int32, (shard, LANES), 0), packed)
        gain_own = jnp.zeros((shard, LANES), F32)
        for q in range(packed):
            cols = pl.ds(pl.multiple_of(y * width + q * LANES, LANES), LANES)
            gain_own = jnp.where(at == q, gain[:, cols], gain_own)
        proj_o[...] = (gain_own * one_term - second) * (float(nz * nx * 2 * img_all) ** -0.5)
        drain(sy.at[pl.ds(0, ny - 1)], sy_s)
        drain(ag.at[0, 0, pl.ds(0, 2), pl.ds(0, nz - 1)], agz_s)
        drain(ag.at[:, 0, pl.ds(0, nx - 1), pl.ds(0, live_z)], agx_s)
        drain(ag.at[0], agc_s)
        drain(st_in, st_s)
        drain(hc.at[:, :, pl.ds(0, live_z)], rc_s)
        drain(hx, rx_s)
        drain(hz.at[:, pl.ds(0, nz - 1)], rz_s)
        drain(ty_in, ty_s)

    sem = pltpu.SemaphoreType.DMA
    pl.run_scoped(
        work,
        pltpu.SemaphoreType.REGULAR,
        pltpu.SemaphoreType.REGULAR,
        sem((9 + in_half,)),
        sem,
        sem,
        *([sem, sem((2,))] * 3),
        *([sem, sem((2,))] * 2),
        sem,
        sem((2, 2)),
        sem,
        sem((2,)),
        sem,
        sem,
    )

    each(in_half, text_last, jnp.where(lax.axis_index("dp_0") < EARLY, in_half, 0))

    cross_t = jnp.sum(cross_f[...], axis=1, keepdims=True)
    inv_t = lax.rsqrt(sq_f[:, 0:1] * per_row + EPS)
    scale_t = inv_t * inv_t * inv_t * (cross_t * per_row)
    for s in range(slices):
        cols = slice(s * tw, (s + 1) * tw)
        text_o[:, cols] = (inv_t * gtxt[s] - txt[:, cols].astype(F32) * scale_t).astype(BF16)

    for way in (0, 1):
        drain(tb.at[way, pl.ds(0, pieces)], ts_s.at[way])


def put_out(text_v, proj_v, text_o, proj_o, sems):
    a = pltpu.make_async_copy(text_v, text_o, sems.at[0])
    b = pltpu.make_async_copy(proj_v, proj_o, sems.at[1])
    a.start()
    b.start()
    a.wait()
    b.wait()


def body(vision_rows, image_count, proj_flat, text_embeds, norm_gain, q_weight, q_grad):
    nz, nx, ny = (lax.axis_size(a) for a in ("dp_0", "dp_1", "mp"))
    total, width = q_weight.shape
    img_all, enc = vision_rows.shape
    text_rows = text_embeds.shape[0]
    shard = proj_flat.shape[0]
    packed = width // LANES
    own_rows = -(-shard // packed // 16) * 16
    near = ny // 2
    slices = 8
    tw = total // slices
    flat_rows = nz * nx * 2 * shard
    sem = pltpu.SemaphoreType.DMA
    any_space = pl.BlockSpec(memory_space=pl.ANY)
    in_vmem = pl.BlockSpec(memory_space=pltpu.VMEM)
    scratch = [
        pltpu.VMEM((total, width), BF16),
        pltpu.VMEM((width, total), BF16),
        pltpu.VMEM((img_all, width), BF16),
        pltpu.VMEM((ny, text_rows, width), BF16),
        pltpu.VMEM((img_all, enc), BF16),
        pltpu.VMEM((enc, img_all), BF16),
        pltpu.VMEM((text_rows, total), BF16),
        pltpu.VMEM((1, total), F32),
        pltpu.VMEM((ny, shard, LANES), BF16),
        pltpu.VMEM((ny, own_rows * packed, LANES), F32),
        pltpu.VMEM((own_rows, total), BF16),
        pltpu.VMEM((2, 2, nx, nz, shard, LANES), BF16),
        pltpu.VMEM((flat_rows, LANES), F32),
        pltpu.VMEM((enc, width), BF16),
        pltpu.VMEM((img_all, width), BF16),
        pltpu.VMEM((2, (near + 1) * slices, text_rows, tw), BF16),
        pltpu.VMEM((slices, text_rows, tw), F32),
        pltpu.VMEM((text_rows, LANES), F32),
        pltpu.VMEM((text_rows, LANES), F32),
        pltpu.VMEM((2, 1, img_all), F32),
        pltpu.VMEM((2, ny - 1, 1, img_all), F32),
        pltpu.VMEM((2, 2, nx, nz, shard, LANES), BF16),
        pltpu.VMEM((2, nx, nz, shard, LANES), BF16),
        pltpu.VMEM((2, nx, nz, shard, LANES), BF16),
        pltpu.VMEM((2, nx - 1, nz, shard, LANES), BF16),
        pltpu.VMEM((2, nz, shard, LANES), BF16),
        pltpu.VMEM((2, nz, shard, LANES), BF16),
        pltpu.VMEM((ny, shard, LANES), BF16),
        pltpu.VMEM((ny - 1, shard, LANES), BF16),
        pltpu.SMEM((ny,), jnp.int32),
        sem((2,)),
        sem((2, (near - 1) * slices // 2 + 1 + slices // 2)),
    ]
    text_v, proj_v = pl.pallas_call(
        functools.partial(kernel, (nz, nx, ny)),
        out_shape=(pltpu.VMEM(text_embeds.shape, BF16), pltpu.VMEM(proj_flat.shape, F32)),
        in_specs=[any_space] * 7,
        out_specs=(in_vmem, in_vmem),
        scratch_shapes=scratch,
        compiler_params=pltpu.CompilerParams(
            collective_id=0,
            has_side_effects=True,
            vmem_limit_bytes=56 * 1024 * 1024,
        ),
        name="step",
    )(vision_rows, image_count, proj_flat, text_embeds, norm_gain.reshape(1, -1), q_weight, q_grad)
    return pl.pallas_call(
        put_out,
        out_shape=(
            jax.ShapeDtypeStruct(text_embeds.shape, BF16),
            jax.ShapeDtypeStruct(proj_flat.shape, F32),
        ),
        in_specs=[in_vmem] * 2,
        out_specs=(any_space, any_space),
        scratch_shapes=[sem((2,))],
        name="put_out",
    )(*(pltpu.with_memory_space_constraint(v, pltpu.VMEM) for v in (text_v, proj_v)))


def solution(mesh):
    finer = Mesh(mesh.devices.reshape(12, 4, 2, mesh.shape["mp"]), ("dp_0", "dp_1", "dp_2", "mp"))
    placed = (P(DP, None), P(DP), P(DP_MP, None), P(DP_MP, None), P(), P(None, "mp"), P(DP, "mp"))
    return jax.shard_map(
        body,
        mesh=finer,
        in_specs=placed,
        out_specs=(P(DP_MP, None), P(DP_MP, None)),
        check_vma=False,
    )
```

```python
import functools

import jax
import jax.numpy as jnp
from jax import lax
from jax.experimental import pallas as pl
from jax.experimental.pallas import tpu as pltpu
from jax.sharding import Mesh
from jax.sharding import PartitionSpec as P

IMG_MAX = 4
PATCH = 8
IMG = IMG_MAX * PATCH
LANES = 128
DP = ("dp_0", "dp_1", "dp_2")
DP_MP = ("dp_0", "dp_1", "dp_2", "mp")
EPS = 1e-05
LEAD = 7
SLACK = 143
EARLY = 3
MESH = pl.DeviceIdType.MESH
F32 = jnp.float32
BF16 = jnp.bfloat16


def dot_nt(a, b):
    return lax.dot_general(a, b, (((1,), (1,)), ((), ())), preferred_element_type=F32)


def kernel(
    sizes,
    vis_h,
    count_h,
    proj_h,
    text_h,
    gain_h,
    qw_h,
    qg_h,
    text_o,
    proj_o,
    qw,
    qi,
    qt,
    vis,
    vis_t,
    txt,
    gain,
    sy,
    rows_f,
    lhs,
    ag,
    flat,
    wblk,
    emb,
    tb,
    gtxt,
    cross_f,
    sq_f,
    st,
    st_in,
    hs,
    hc,
    h1,
    hx,
    h2,
    hz,
    ty,
    ty_in,
    count_s,
    ts_s,
    ts_r,
):
    nz, nx, ny = sizes
    text_rows, total = txt.shape
    near = ny // 2
    slices = gtxt.shape[0]
    in_half = slices // 2
    tw = tb.shape[3]
    per_row = 1.0 / total
    pieces = 2 * in_half + (ny - 3) * in_half
    mid_sems = (near - 1) * slices // 2

    def drain(ref, sem):
        pltpu.make_async_copy(ref, ref, sem).wait()

    def each(n, act, lo=0):
        def one(k, carry):
            act(k)
            return carry

        lax.fori_loop(lo, n, one, 0)

    def arrival(way, d, h, k):
        mid = ((d - 1) * slices + h * in_half + k) // 2
        end = mid_sems + jnp.where(h == way, 1 + k, 0)
        return ts_r.at[way, jnp.where(d > 0, mid, end)]

    def text_last(k):
        for h in (0, 1):
            s = h * in_half + k
            drain(tb.at[h, 0], arrival(h, 0, h, k))
            cols = pl.ds(pl.multiple_of(s * tw, LANES), tw)
            g = (gtxt[s] + tb[h, s].astype(F32)) * gain[:, cols]
            gtxt[s] = g
            prod = g * txt[:, cols].astype(F32)
            for q in range(tw // LANES):
                cross_f[...] += prod[:, q * LANES : (q + 1) * LANES]

    def work(
        in_sem,
        y_sem,
        load_sem,
        sy_s,
        sy_r,
        agz_s,
        agz_r,
        agx_s,
        agx_r,
        agc_s,
        agc_r,
        st_s,
        st_r,
        rc_s,
        rc_r,
        rx_s,
        rx_r,
        rz_s,
        rz_r,
        ty_s,
        ty_r,
    ):
        z = lax.axis_index("dp_0")
        x = lax.axis_index("dp_1")
        c = lax.axis_index("dp_2")
        y = lax.axis_index("mp")
        width = qw.shape[1]
        enc = vis.shape[1]
        img_all = qi.shape[0]
        packed = width // LANES
        shard = proj_h.shape[0]
        own_rows = lhs.shape[0]
        live_z = -(-enc * packed // (2 * nx * shard))
        other = 1 - c

        def ring(i, n):
            return lax.rem(i, n)

        def begin(make, n):
            def one(i, carry):
                side = jnp.where(lax.rem(i, 2) == 1, (i + 1) // 2, -(i // 2))
                make(n // 2 + side).start()
                return carry

            lax.fori_loop(0, n - 1, one, 0)

        def send(src, dst, send_sem, recv_sem, axis, index):
            return pltpu.make_async_remote_copy(
                src_ref=src,
                dst_ref=dst,
                send_sem=send_sem,
                recv_sem=recv_sem,
                device_id={axis: index},
                device_id_type=MESH,
            )

        def load(src, dst, i):
            return pltpu.make_async_copy(src, dst, load_sem.at[i])

        rows_each = IMG + text_rows

        def text_in(k, i):
            base = pl.multiple_of(k * rows_each + IMG, 16)
            return load(qg_h.at[pl.ds(base, text_rows)], qt.at[k], i)

        def img_in(k):
            base = pl.multiple_of(k * rows_each, 16)
            to = qi.at[pl.ds(pl.multiple_of(k * IMG, 16), IMG)]
            return load(qg_h.at[pl.ds(base, IMG)], to, 7)

        def slice_in(s, own=None):
            cols = pl.ds(pl.multiple_of(s * tw, tw), tw)
            return load(qw_h.at[cols], qw.at[cols], 9 + lax.rem(s, in_half) if own is None else own)

        def pair_wait(i):
            drain(qw.at[pl.ds(0, 2 * tw)], load_sem.at[9 + i])

        slice_in(0).start()
        text_in(ring(y + near, ny), 5).start()
        slice_in(in_half, 9 + in_half).start()
        load(proj_h, ag.at[0, c, x, z], 0).start()
        load(proj_h, sy.at[y], 1).start()

        barrier = pltpu.get_barrier_semaphore()

        def tell(what, axis, index):
            pl.semaphore_signal(what, inc=1, device_id={axis: index}, device_id_type=MESH)

        corner_z = ((x == 0) & (y == 0) & (c == 0)).astype(jnp.int32)
        corner_x = ((z == 0) & (y == 0) & (c == 0)).astype(jnp.int32)
        corner_y = ((z == 0) & (x == 0) & (c == 0)).astype(jnp.int32)
        rank_z = ring(z + nz - corner_z, nz)
        rank_x = ring(x + nx - corner_x, nx)

        def tell_z(what):
            return lambda r: tell(what, "dp_0", ring(r + corner_z, nz))

        def tell_x(what):
            return lambda r: tell(what, "dp_1", ring(r + corner_x, nx))

        def turn(v):
            place = jnp.where(v < near, v, ny + near - 1 - v)
            place = jnp.where(place == near, near - 1, jnp.where(place == near - 1, near, place))
            return ring(place + ny - corner_y, ny)

        def awaits(a, b, j):
            return (turn(b) < turn(a)) | (j == 1) | (j == ny - 1)

        y_now = jnp.int32(0)
        for j in range(1, ny):
            v = ring(y + j, ny)
            y_now = y_now + awaits(y, v, j).astype(jnp.int32)

            @pl.when(awaits(v, y, j))
            def _(v=v):
                tell(barrier, "mp", v)

        each(nz, tell_z(barrier), rank_z + 1)
        each(nx, tell_x(barrier), rank_x + 1)

        @pl.when(c == 1)
        def _():
            tell(barrier, "dp_2", other)

        def next_slices(i):
            slice_in(i).start()
            slice_in(in_half + i).start()

        each(in_half, next_slices, 1)
        each(ny, lambda j: text_in(ring(y + near + j, ny), 6).start(), 1)
        load(gain_h, gain, 4).start()
        load(vis_h, vis, 2).start()
        each(ny, lambda k: img_in(k).start())
        load(text_h, txt, 3).start()
        load(count_h, count_s, 8).start()

        def owner_of(way, d):
            return ring(y + d, ny) if way == 0 else ring(y + ny - d, ny)

        def text_dot(owner, s):
            cols = qw[pl.ds(pl.multiple_of(s * tw, tw), tw), :]
            return dot_nt(qt[owner], cols)

        def text_send(way, d, h, k):
            s = h * in_half + k
            return send(
                tb.at[way, d * slices + s],
                tb.at[way, (d - 1) * slices + s],
                ts_s.at[way],
                arrival(way, d - 1, h, k),
                "mp",
                ring(y + 1, ny) if way == 0 else ring(y + ny - 1, ny),
            )

        def text_first(i):
            far = i < in_half
            k = lax.rem(i, in_half)
            for way in (0, 1):
                h = jnp.where(far, way, 1 - way)
                d = jnp.where(far, near, near - 1)
                s = h * in_half + k
                tb[way, d * slices + s] = text_dot(owner_of(way, d), s).astype(BF16)
                text_send(way, d, h, k).start()

        def text_next_first(i):
            @pl.when(i < in_half)
            def _():
                pair_wait(i)

            text_first(i)

        def text_relay(n):
            u = n // in_half
            k = lax.rem(n, in_half)
            d = near - 1 - (u + 1) // 2
            for way in (0, 1):
                h = lax.rem(u + way, 2)
                s = h * in_half + k
                slot = d * slices + s
                mine = text_dot(owner_of(way, d), s)

                @pl.when(lax.rem(k, 2) == 0)
                def _(way=way, d=d, h=h, k=k):
                    drain(tb.at[way, pl.ds(0, 2)], arrival(way, d, h, k))

                tb[way, slot] = (mine + tb[way, slot].astype(F32)).astype(BF16)
                text_send(way, d, h, k).start()

        steps = (ny - 3) * in_half
        firsts = 2 * in_half
        place = jnp.where(y < near, y, ny + near - 1 - y)
        begins = jnp.where(z < 7, 35 + 14 * z, 110 + 3 * z)
        begins += jnp.where(y < near, 6 * y - 30, 3 * (place - near) - 10)
        begins += jnp.where(x < 2, 5 * x - 10, 0) - 4 * c
        ahead = jnp.clip((SLACK - begins) // 21, 0, LEAD)
        out = [jnp.int32(1), 1]

        def pace(n, most=None, times=1, more=0):
            most = min(n + LEAD if most is None else most, pieces)
            upto = jnp.minimum(n + times * ahead + more, most)
            upto = jnp.maximum(upto, out[0])
            if out[1] < firsts:
                each(jnp.minimum(upto, firsts), text_next_first, jnp.minimum(out[0], firsts))
            if most > firsts:
                each(jnp.maximum(upto, firsts) - firsts, text_relay, jnp.maximum(out[0], firsts) - firsts)
            out[0], out[1] = upto, max(out[1], min(n, pieces))

        def text_near(k):
            @pl.when(k == 0)
            def _():
                for way in (0, 1):
                    drain(tb.at[way, pl.ds(0, in_half)], arrival(way, 0, 1 - way, 0))

            for h in (0, 1):
                s = h * in_half + k
                gtxt[s] = text_dot(y, s) + tb[1 - h, s].astype(F32)

        def agz(k):
            ref = ag.at[k, c, x, z]
            return lambda j: send(ref, ref, agz_s, agz_r.at[k], "dp_0", ring(z + j, nz))

        def agx(k):
            ref = ag.at[k, c, x, pl.ds(0, live_z)]
            return lambda j: send(ref, ref, agx_s, agx_r.at[k], "dp_1", ring(x + j, nx))

        def agc(k):
            ref = ag.at[k, c]
            return send(ref, ref, agc_s, agc_r.at[k], "dp_2", other)

        def agz_wait(k):
            drain(ag.at[0, 0, 0, pl.ds(0, nz - 1)], agz_r.at[k])

        def agx_wait(k):
            drain(ag.at[0, 0, pl.ds(0, nx - 1), pl.ds(0, live_z)], agx_r.at[k])

        def agc_wait(k):
            drain(ag.at[0, 0], agc_r.at[k])

        def rc(k):
            live = pl.ds(0, live_z)
            return send(
                hs.at[k, other, :, live], hc.at[k, :, live], rc_s, rc_r.at[k], "dp_2", other
            )

        side_z = min(2, (nz - 1) // 2)
        near_z = 2 * side_z + 1
        runs = (pl.ds(near_z, nz - near_z), pl.ds(0, near_z))
        FAR, NEAR = 0, 1

        def slot_z(zz):
            return ring(zz - z + side_z + nz, nz)

        def rx(k, part):
            def one(j):
                to = ring(x + j, nx)
                src, dst = h1.at[k, to, runs[part]], hx.at[k, j - 1, runs[part]]
                return send(src, dst, rx_s, rx_r.at[k, part], "dp_1", to)

            begin(one, nx)

        def rz(k, part):
            def one(off):
                to = ring(z + off + nz, nz)
                return send(
                    h2.at[k, off + side_z], hz.at[k, off + side_z], rz_s, rz_r.at[k], "dp_0", to
                )

            if part == NEAR:
                for off in range(side_z, 0, -1):
                    one(off).start()
                    one(-off).start()
                return

            def by_side(i):
                one(nz // 2 + jnp.where(lax.rem(i, 2) == 1, (i + 1) // 2, -(i // 2))).start()

            each(nz - near_z, by_side)

        def st_send(k):
            return lambda j: send(
                st.at[k], st_in.at[k, j - 1], st_s, st_r.at[k], "mp", ring(y + j, ny)
            )

        def sy_send(j):
            return send(sy.at[y], sy.at[y], sy_s, sy_r, "mp", ring(y + j, ny))

        def ty_send(j):
            to = ring(y + j, ny)
            return send(ty.at[to], ty_in.at[j - 1], ty_s, ty_r, "mp", to)

        def place(zz, r):
            return pl.ds(pl.multiple_of((zz * 2 * nx + r) * shard, 16), shard)

        def unpack(k):
            def one(zz):
                for r in range(2 * nx):
                    flat[place(zz, r), :] = ag[k, r % 2, r // 2, zz].astype(F32)

            each(live_z, one)
            for q in range(packed):
                wblk[:, q * LANES : (q + 1) * LANES] = flat[pl.ds(q, enc, packed), :].astype(BF16)

        def pack(k, block):
            for q in range(packed):
                flat[pl.ds(q, enc, packed), :] = block[:, q * LANES : (q + 1) * LANES]
            end = live_z * 2 * nx * shard
            if end > enc * packed:
                flat[enc * packed : end, :] = jnp.zeros((end - enc * packed, LANES), F32)

            def one(zz):
                for r in range(2 * nx):
                    hs[k, r % 2, r // 2, zz] = flat[place(zz, r), :].astype(BF16)

            each(live_z, one)

        def core_sum(k):
            rc(k).wait_recv()

            def one(zz):
                for xx in range(nx):
                    pair = hs[k, c, xx, zz].astype(F32) + hc[k, xx, zz].astype(F32)
                    h1[k, xx, slot_z(zz)] = pair.astype(BF16)

            each(live_z, one)

        def x_sum(k, part):
            drain(hx.at[k, :, runs[part]], rx_r.at[k, part])

            def one(slot):
                acc = h1[k, x, slot].astype(F32)
                for j in range(nx - 1):
                    acc = acc + hx[k, j, slot].astype(F32)
                h2[k, slot] = acc.astype(BF16)

            lo, hi = (near_z, nz) if part == FAR else (0, near_z)
            each(hi, one, lo)
            rz(k, part)

        def z_sum(k):
            drain(hz.at[k, pl.ds(0, nz - 1)], rz_r.at[k])
            acc = h2[k, side_z].astype(F32)
            for slot in range(nz):
                if slot != side_z:
                    acc = acc + hz[k, slot].astype(F32)
            return acc

        def publish(k, column):
            wide = jnp.broadcast_to(column, (img_all, LANES))
            st[k] = wide.T[0:1, :]
            begin(st_send(k), ny)

        def collected(k):
            drain(st_in.at[k], st_r.at[k])
            row = st[k]
            for j in range(ny - 1):
                row = row + st_in[k, j]
            return jnp.broadcast_to(row, (LANES, img_all)).T[:, 0:1]

        def text_ahead(way):
            tb[way, near * slices + way * in_half] = text_dot(owner_of(way, near), way * in_half).astype(BF16)

        last = y == near
        text_in(ring(y + near, ny), 5).wait()

        def ahead_of(way):
            slice_in(way * in_half, 9 + way * in_half).wait()
            text_ahead(way)

        def in_turn(first):
            def then():
                for way in (first, 1 - first):
                    if way != first:
                        ahead_of(way)
                    text_send(way, near, way, 0).start()

            return then

        pl.when(last)(lambda: ahead_of(1))
        pl.when(jnp.logical_not(last))(lambda: ahead_of(0))
        pl.semaphore_wait(barrier, y_now + rank_z + rank_x + other)
        each(rank_z, tell_z(in_sem))
        pl.when(last)(in_turn(1))
        pl.when(jnp.logical_not(last))(in_turn(0))
        each(rank_x, tell_x(in_sem))
        load(proj_h, sy.at[y], 1).wait()

        @pl.when(c == 0)
        def _():
            tell(in_sem, "dp_2", other)

        for j in range(1, ny):
            v = ring(y + j, ny)

            @pl.when(jnp.logical_not(awaits(v, y, j)))
            def _(v=v):
                tell(y_sem, "mp", v)

        load(proj_h, ag.at[0, c, x, z], 0).wait()
        drain(qt.at[pl.ds(0, ny - 1)], load_sem.at[6])

        early = z < EARLY
        pace(1, 3, 0, (ny - 1 - turn(y)) // 3)

        @pl.when(y_now < ny - 1)
        def _():
            pl.semaphore_wait(y_sem, ny - 1 - y_now)

        begin(sy_send, ny)
        pace(1, firsts + 2, 2)
        rest = (nz - 1 - rank_z) + (nx - 1 - rank_x) + c

        @pl.when(rest > 0)
        def _():
            pl.semaphore_wait(in_sem, rest)

        begin(agz(0), nz)
        rows_f[...] = jnp.zeros(rows_f.shape, F32)
        cross_f[...] = jnp.zeros(cross_f.shape, F32)
        for k in (0, 1):
            for zz in range(live_z, nz):
                h1[k, :, slot_z(zz)] = jnp.zeros((nx, shard, LANES), BF16)
        pace(4)
        load(vis_h, vis, 2).wait()
        vis_t[...] = vis[...].T
        pace(6)
        agz_wait(0)
        begin(agx(0), nx)

        load(gain_h, gain, 4).wait()
        drain(sy.at[pl.ds(0, ny - 1)], sy_r)
        for m in range(ny):
            rows_f[m, 0:shard, :] = sy[m].astype(F32)
            for q in range(packed):
                cols = slice(m * width + q * LANES, m * width + (q + 1) * LANES)
                piece = rows_f[m, pl.ds(q, own_rows, packed), :] * gain[:, cols]
                lhs[:, cols] = piece.astype(BF16)
        prod = jnp.dot(lhs[...], qw[...], preferred_element_type=F32)
        for q in range(packed):
            rows_f[0, pl.ds(q, own_rows, packed), :] = prod[:, q * LANES : (q + 1) * LANES]
        ag[1, c, x, z] = rows_f[0, 0:shard, :].astype(BF16)
        begin(agz(1), nz)
        pace(9)
        agx_wait(0)
        agc(0).start()

        drain(qi, load_sem.at[7])
        agz_wait(1)
        begin(agx(1), nx)
        agc_wait(0)
        unpack(0)
        embed = jnp.dot(vis[...], wblk[...], preferred_element_type=F32).astype(BF16)
        emb[...] = embed
        embed = embed.astype(F32)
        publish(0, jnp.sum(embed * embed, axis=1, keepdims=True))
        pace(13)

        agx_wait(1)
        agc(1).start()
        agc_wait(1)
        unpack(1)
        back = jnp.dot(vis[...], wblk[...], preferred_element_type=F32)
        publish(1, jnp.sum(back * qi[...].astype(F32), axis=1, keepdims=True))
        pace(14)

        load(count_h, count_s, 8).wait()
        row = lax.broadcasted_iota(jnp.int32, (img_all, 1), 0)
        counts = jnp.zeros((img_all, 1), jnp.int32)
        for k in range(ny):
            counts = jnp.where(row // IMG == k, count_s[k], counts)
        live = lax.rem(row, IMG) // PATCH < counts
        inv = lax.rsqrt(collected(0) * per_row + EPS)
        left = jnp.where(live, inv * qi[...].astype(F32), 0.0).astype(BF16)
        pack(0, jnp.dot(vis_t[...], left, preferred_element_type=F32))
        rc(0).start()
        pace(16)
        core_sum(0)
        rx(0, FAR)
        rx(0, NEAR)
        pace(17)

        mean = collected(1) * per_row
        right = jnp.where(live, (inv * inv * inv * mean) * emb[...].astype(F32), 0.0).astype(BF16)
        pack(1, jnp.dot(vis_t[...], right, preferred_element_type=F32))
        rc(1).start()
        pace(19)
        core_sum(1)
        rx(1, FAR)
        rx(1, NEAR)
        x_sum(0, FAR)
        pace(20)

        load(text_h, txt, 3).wait()
        sq_t = jnp.zeros((text_rows, 1), F32)
        for s in range(slices):
            rows_t = txt[:, s * tw : (s + 1) * tw].astype(F32)
            sq_t = sq_t + jnp.sum(rows_t * rows_t, axis=1, keepdims=True)
        sq_f[...] = jnp.broadcast_to(sq_t, sq_f.shape)
        x_sum(0, NEAR)
        pace(22)
        x_sum(1, FAR)
        pace(24, pieces - 2)

        rows_f[0, 0:shard, :] = z_sum(0)
        for q in range(packed):
            lhs[:, q * LANES : (q + 1) * LANES] = rows_f[0, pl.ds(q, own_rows, packed), :].astype(BF16)
        term = lhs[:, 0:width]
        for m in range(ny):
            prod = dot_nt(term, qw[m * width : (m + 1) * width, :])
            for q in range(packed):
                rows_f[m, pl.ds(q, own_rows, packed), :] = prod[:, q * LANES : (q + 1) * LANES]
            ty[m] = rows_f[m, 0:shard, :].astype(BF16)
        begin(ty_send, ny)
        x_sum(1, NEAR)
        pace(pieces)
        each(in_half, text_near)
        first_part = jnp.where(early, in_half, 0)
        each(first_part, text_last)
        second = z_sum(1)
        drain(ty_in, ty_r)
        one_term = ty[y].astype(F32)
        for j in range(ny - 1):
            one_term = one_term + ty_in[j].astype(F32)
        at = lax.rem(lax.broadcasted_iota(jnp.int32, (shard, LANES), 0), packed)
        gain_own = jnp.zeros((shard, LANES), F32)
        for q in range(packed):
            cols = pl.ds(pl.multiple_of(y * width + q * LANES, LANES), LANES)
            gain_own = jnp.where(at == q, gain[:, cols], gain_own)
        proj_o[...] = (gain_own * one_term - second) * (float(nz * nx * 2 * img_all) ** -0.5)
        drain(sy.at[pl.ds(0, ny - 1)], sy_s)
        drain(ag.at[0, 0, pl.ds(0, 2), pl.ds(0, nz - 1)], agz_s)
        drain(ag.at[:, 0, pl.ds(0, nx - 1), pl.ds(0, live_z)], agx_s)
        drain(ag.at[0], agc_s)
        drain(st_in, st_s)
        drain(hc.at[:, :, pl.ds(0, live_z)], rc_s)
        drain(hx, rx_s)
        drain(hz.at[:, pl.ds(0, nz - 1)], rz_s)
        drain(ty_in, ty_s)

    sem = pltpu.SemaphoreType.DMA
    pl.run_scoped(
        work,
        pltpu.SemaphoreType.REGULAR,
        pltpu.SemaphoreType.REGULAR,
        sem((10 + in_half,)),
        sem,
        sem,
        *([sem, sem((2,))] * 3),
        *([sem, sem((2,))] * 2),
        sem,
        sem((2, 2)),
        sem,
        sem((2,)),
        sem,
        sem,
    )

    each(in_half, text_last, jnp.where(lax.axis_index("dp_0") < EARLY, in_half, 0))

    cross_t = jnp.sum(cross_f[...], axis=1, keepdims=True)
    inv_t = lax.rsqrt(sq_f[:, 0:1] * per_row + EPS)
    scale_t = inv_t * inv_t * inv_t * (cross_t * per_row)
    for s in range(slices):
        cols = slice(s * tw, (s + 1) * tw)
        text_o[:, cols] = (inv_t * gtxt[s] - txt[:, cols].astype(F32) * scale_t).astype(BF16)

    for way in (0, 1):
        drain(tb.at[way, pl.ds(0, pieces)], ts_s.at[way])


def put_out(text_v, proj_v, text_o, proj_o, sems):
    a = pltpu.make_async_copy(text_v, text_o, sems.at[0])
    b = pltpu.make_async_copy(proj_v, proj_o, sems.at[1])
    a.start()
    b.start()
    a.wait()
    b.wait()


def body(vision_rows, image_count, proj_flat, text_embeds, norm_gain, q_weight, q_grad):
    nz, nx, ny = (lax.axis_size(a) for a in ("dp_0", "dp_1", "mp"))
    total, width = q_weight.shape
    img_all, enc = vision_rows.shape
    text_rows = text_embeds.shape[0]
    shard = proj_flat.shape[0]
    packed = width // LANES
    own_rows = -(-shard // packed // 16) * 16
    near = ny // 2
    slices = 8
    tw = total // slices
    flat_rows = nz * nx * 2 * shard
    sem = pltpu.SemaphoreType.DMA
    any_space = pl.BlockSpec(memory_space=pl.ANY)
    in_vmem = pl.BlockSpec(memory_space=pltpu.VMEM)
    scratch = [
        pltpu.VMEM((total, width), BF16),
        pltpu.VMEM((img_all, width), BF16),
        pltpu.VMEM((ny, text_rows, width), BF16),
        pltpu.VMEM((img_all, enc), BF16),
        pltpu.VMEM((enc, img_all), BF16),
        pltpu.VMEM((text_rows, total), BF16),
        pltpu.VMEM((1, total), F32),
        pltpu.VMEM((ny, shard, LANES), BF16),
        pltpu.VMEM((ny, own_rows * packed, LANES), F32),
        pltpu.VMEM((own_rows, total), BF16),
        pltpu.VMEM((2, 2, nx, nz, shard, LANES), BF16),
        pltpu.VMEM((flat_rows, LANES), F32),
        pltpu.VMEM((enc, width), BF16),
        pltpu.VMEM((img_all, width), BF16),
        pltpu.VMEM((2, (near + 1) * slices, text_rows, tw), BF16),
        pltpu.VMEM((slices, text_rows, tw), F32),
        pltpu.VMEM((text_rows, LANES), F32),
        pltpu.VMEM((text_rows, LANES), F32),
        pltpu.VMEM((2, 1, img_all), F32),
        pltpu.VMEM((2, ny - 1, 1, img_all), F32),
        pltpu.VMEM((2, 2, nx, nz, shard, LANES), BF16),
        pltpu.VMEM((2, nx, nz, shard, LANES), BF16),
        pltpu.VMEM((2, nx, nz, shard, LANES), BF16),
        pltpu.VMEM((2, nx - 1, nz, shard, LANES), BF16),
        pltpu.VMEM((2, nz, shard, LANES), BF16),
        pltpu.VMEM((2, nz, shard, LANES), BF16),
        pltpu.VMEM((ny, shard, LANES), BF16),
        pltpu.VMEM((ny - 1, shard, LANES), BF16),
        pltpu.SMEM((ny,), jnp.int32),
        sem((2,)),
        sem((2, (near - 1) * slices // 2 + 1 + slices // 2)),
    ]
    text_v, proj_v = pl.pallas_call(
        functools.partial(kernel, (nz, nx, ny)),
        out_shape=(pltpu.VMEM(text_embeds.shape, BF16), pltpu.VMEM(proj_flat.shape, F32)),
        in_specs=[any_space] * 7,
        out_specs=(in_vmem, in_vmem),
        scratch_shapes=scratch,
        compiler_params=pltpu.CompilerParams(
            collective_id=0,
            has_side_effects=True,
            vmem_limit_bytes=56 * 1024 * 1024,
        ),
        name="step",
    )(vision_rows, image_count, proj_flat, text_embeds, norm_gain.reshape(1, -1), q_weight, q_grad)
    return pl.pallas_call(
        put_out,
        out_shape=(
            jax.ShapeDtypeStruct(text_embeds.shape, BF16),
            jax.ShapeDtypeStruct(proj_flat.shape, F32),
        ),
        in_specs=[in_vmem] * 2,
        out_specs=(any_space, any_space),
        scratch_shapes=[sem((2,))],
        name="put_out",
    )(*(pltpu.with_memory_space_constraint(v, pltpu.VMEM) for v in (text_v, proj_v)))


def solution(mesh):
    finer = Mesh(mesh.devices.reshape(12, 4, 2, mesh.shape["mp"]), ("dp_0", "dp_1", "dp_2", "mp"))
    placed = (P(DP, None), P(DP), P(DP_MP, None), P(DP_MP, None), P(), P(None, "mp"), P(DP, "mp"))
    return jax.shard_map(
        body,
        mesh=finer,
        in_specs=placed,
        out_specs=(P(DP_MP, None), P(DP_MP, None)),
        check_vma=False,
    )
```
